32 devices in a mesh: tp: 8 (over z, y), ep: 4 (over x, core).
Axes of the slice: x: 2, y: 2, z: 4, core: 2. Of those that a mesh axis runs over, the one named last changes fastest.
Arguments:
- tokens: bfloat16 [16384, 512], P('ep')
- w_router: float32 [512, 32], replicated
- expert_idx: int32 [16384, 2], P('ep')
- slot_idx: int32 [16384, 2], P('ep')
- w_gelu: bfloat16 [32, 512, 1024], P('ep', None, 'tp')
- w_linear: bfloat16 [32, 512, 1024], P('ep', None, 'tp')
- w_out: bfloat16 [32, 1024, 512], P('ep', 'tp')
- dy_tokens: bfloat16 [16384, 512], P('ep')
Outputs:
- output 1: bfloat16 [16384, 512], P('ep')
- output 2: bfloat16 [16384, 512], P('ep')
- output 3: bfloat16 [32, 512, 1024], P('ep', None, 'tp')
- output 4: bfloat16 [32, 512, 1024], P('ep', None, 'tp')
- output 5: bfloat16 [32, 1024, 512], P('ep', 'tp')
- output 6: float32 [512, 32], replicated
- output 7: float32 [], replicated
All inputs are finite; a program needn't handle non-finite values.
Results may differ from the reference program's by a relative error of at most 0.0160283.
Values are sent between devices in bfloat16 or wider.
A program may use at most 1 GiB of HBM per device.

```python
import jax
import jax.numpy as jnp
from jax import lax

D_MODEL = 512
D_FF = 1024
EXPERTS = 32
CAPACITY = 512
SHARDS = 4
TOKENS_SHARD = CAPACITY * EXPERTS // 4
TOKENS = TOKENS_SHARD * SHARDS


def cold_expert(offset, cold_index):
    return (offset + 8 * (cold_index // 7) + 1 + cold_index % 7) % EXPERTS


def draw_routes(rng_key):
    key_hot, key_perm, key_one, key_two = jax.random.split(rng_key, 4)
    hot_count = EXPERTS // 8
    per_hot = CAPACITY + CAPACITY // 8
    cold_count = EXPERTS - hot_count
    offset = jax.random.randint(key_hot, (), 0, 8)
    position = jnp.arange(TOKENS_SHARD)
    hot_first = (offset + 8 * (position // per_hot)) % EXPERTS
    free_first = jax.random.randint(key_one, (TOKENS_SHARD,), 0, EXPERTS)
    first_sorted = jnp.where(position < hot_count * per_hot, hot_first, free_first)
    token_order = jax.random.permutation(key_perm, TOKENS_SHARD)
    top_one = first_sorted[token_order]
    cold_pick = jax.random.randint(key_two, (TOKENS_SHARD,), 0, cold_count)
    top_two = cold_expert(offset, cold_pick)
    top_two = jnp.where(top_two == top_one, cold_expert(offset, (cold_pick + 1) % cold_count), top_two)
    expert_ids = jnp.arange(EXPERTS)
    one_hot = (top_one[:, None] == expert_ids).astype(jnp.int32)
    two_hot = (top_two[:, None] == expert_ids).astype(jnp.int32)
    one_rank = jnp.cumsum(one_hot, axis=0) - one_hot
    two_rank = jnp.cumsum(two_hot, axis=0) - two_hot + jnp.sum(one_hot, axis=0)
    slot_one = jnp.sum(one_rank * one_hot, axis=1)
    slot_two = jnp.sum(two_rank * two_hot, axis=1)
    choices = jnp.stack([top_one, top_two], axis=1).astype(jnp.int32)
    slot_pairs = jnp.stack([slot_one, slot_two], axis=1).astype(jnp.int32)
    return choices, slot_pairs


def setup_inputs(seed: int = 0) -> dict:
    root_key = jax.random.key(seed)
    sub_keys = jax.random.split(root_key, 8)
    tokens = jax.random.normal(sub_keys[0], (TOKENS, D_MODEL), jnp.float32).astype(jnp.bfloat16)
    w_router = jax.random.normal(sub_keys[1], (D_MODEL, EXPERTS), jnp.float32) * (1.5 * D_MODEL ** -0.5)
    route_keys = jax.random.split(sub_keys[2], SHARDS)
    choices, slot_pairs = jax.vmap(draw_routes)(route_keys)
    w_gelu = (jax.random.normal(sub_keys[3], (EXPERTS, D_MODEL, D_FF), jnp.float32) * D_MODEL ** -0.5).astype(jnp.bfloat16)
    w_linear = (jax.random.normal(sub_keys[4], (EXPERTS, D_MODEL, D_FF), jnp.float32) * D_MODEL ** -0.5).astype(jnp.bfloat16)
    w_out = (jax.random.normal(sub_keys[5], (EXPERTS, D_FF, D_MODEL), jnp.float32) * D_FF ** -0.5).astype(jnp.bfloat16)
    dy_tokens = jax.random.normal(sub_keys[6], (TOKENS, D_MODEL), jnp.float32).astype(jnp.bfloat16)
    return {"tokens": tokens, "w_router": w_router, "expert_idx": choices.reshape(TOKENS, 2), "slot_idx": slot_pairs.reshape(TOKENS, 2), "w_gelu": w_gelu, "w_linear": w_linear, "w_out": w_out, "dy_tokens": dy_tokens}


def gated_gelu(pre_gelu, pre_lin):
    return jax.nn.gelu(pre_gelu, approximate=True) * pre_lin


def moe_forward(tokens, w_router, w_gelu, w_linear, w_out, expert_idx, slot_idx):
    expert_ids = jnp.arange(EXPERTS)
    logits = jnp.dot(tokens.astype(jnp.float32), w_router)
    prob_rows = jax.nn.softmax(logits, axis=-1)
    choice_hot = (expert_idx[:, :, None] == expert_ids).astype(jnp.float32)
    picked = jnp.einsum("te,tke->tk", prob_rows, choice_hot)
    gate_vals = picked / jnp.sum(picked, axis=1, keepdims=True)
    flat_pos = jnp.where(slot_idx < CAPACITY, expert_idx * CAPACITY + slot_idx, EXPERTS * CAPACITY)
    shard_pos = flat_pos.reshape(SHARDS, 2 * TOKENS_SHARD)
    shard_rows = tokens.reshape(SHARDS, TOKENS_SHARD, D_MODEL)

    def fill_buffer(packed):
        pos_row, buf_rows = packed
        filled = jax.ops.segment_sum(jnp.repeat(buf_rows, 2, axis=0), pos_row, num_segments=EXPERTS * CAPACITY + 1)
        return filled[: EXPERTS * CAPACITY]

    buffers = lax.map(fill_buffer, (shard_pos, shard_rows))
    expert_rows = jnp.moveaxis(buffers.reshape(SHARDS, EXPERTS, CAPACITY, D_MODEL), 1, 0)

    def expert_ffn(packed):
        buf_rows, gelu_w, lin_w, out_w = packed
        rows_wide = buf_rows.reshape(SHARDS * CAPACITY, D_MODEL).astype(jnp.float32)
        pre_gelu = jnp.dot(rows_wide, gelu_w.astype(jnp.float32))
        pre_lin = jnp.dot(rows_wide, lin_w.astype(jnp.float32))
        hidden = gated_gelu(pre_gelu, pre_lin).astype(jnp.bfloat16)
        result = jnp.dot(hidden.astype(jnp.float32), out_w.astype(jnp.float32)).astype(jnp.bfloat16)
        return result.reshape(SHARDS, CAPACITY, D_MODEL)

    outputs = lax.map(expert_ffn, (expert_rows, w_gelu, w_linear, w_out))
    back_rows = jnp.moveaxis(outputs, 0, 1).reshape(SHARDS, EXPERTS * CAPACITY, D_MODEL)

    def gather_rows(packed):
        src_table, pos_row = packed
        return jnp.take(src_table, pos_row, axis=0, mode="fill", fill_value=0)

    chosen = lax.map(gather_rows, (back_rows, shard_pos)).reshape(TOKENS, 2, D_MODEL)
    y_out = jnp.einsum("tk,tkd->td", gate_vals, chosen.astype(jnp.float32)).astype(jnp.bfloat16)
    top_frac = jnp.mean(choice_hot[:, 0, :], axis=0)
    aux_loss = EXPERTS * jnp.sum(top_frac * jnp.mean(prob_rows, axis=0))
    return y_out, aux_loss


def reference(tokens, w_router, expert_idx, slot_idx, w_gelu, w_linear, w_out, dy_tokens):
    def layer_fn(x_in, router, gelu_w, lin_w, out_w):
        return moe_forward(x_in, router, gelu_w, lin_w, out_w, expert_idx, slot_idx)

    (y_out, aux_loss), pullback = jax.vjp(layer_fn, tokens, w_router, w_gelu, w_linear, w_out)
    grad_x, grad_router, grad_gelu, grad_lin, grad_out = pullback((dy_tokens, jnp.asarray(0.01, jnp.float32)))
    return y_out, grad_x, grad_gelu, grad_lin, grad_out, grad_router, aux_loss
```

```python
import functools

import jax
import jax.numpy as jnp
from jax import lax
from jax.experimental import pallas as pl
from jax.experimental.pallas import tpu as pltpu
from jax.sharding import PartitionSpec as P

AUX_WEIGHT = 0.01
F32 = jnp.float32
BF16 = jnp.bfloat16
VMEM_LIMIT = 64000 * 1024
GELU_C = 0.7978845608028654
GELU_A = 0.044715
ANY = pl.ANY


def dot_nn(a, b):
    return lax.dot_general(a, b, (((1,), (0,)), ((), ())), preferred_element_type=F32)


def dot_nt(a, b):
    return lax.dot_general(a, b, (((1,), (1,)), ((), ())), preferred_element_type=F32)


def dot_tn(a, b):
    return lax.dot_general(a, b, (((0,), (0,)), ((), ())), preferred_element_type=F32)


def split3(v):
    hi = v.astype(BF16)
    rest = v - hi.astype(F32)
    mid = rest.astype(BF16)
    lo = (rest - mid.astype(F32)).astype(BF16)
    return hi, mid, lo


def remote(src, dst, send_sem, recv_sem, tp, ep):
    return pltpu.make_async_remote_copy(
        src_ref=src, dst_ref=dst, send_sem=send_sem, recv_sem=recv_sem,
        device_id={"tp": tp, "ep": ep}, device_id_type=pl.DeviceIdType.MESH,
    )


def dispatch_kernel(n_tp, n_ep, cap, x_ref, dy_ref, idx_ref, key_ref, wgt_ref, w0_ref, w1_ref, wo_ref,
                    r_out, d_out, w0_out, w1_out, wo_out, prob_out, gate_out, stat_out,
                    rbuf, dbuf, stat_buf, acc_r, acc_d, w_send, w_recv, row_send, row_recv, st_send, st_recv, loc_sem):
    s = lax.axis_index("tp")
    q = lax.axis_index("ep")
    tokens = x_ref.shape[0]
    experts = n_tp * n_ep
    weights = ((w0_ref, w0_out), (w1_ref, w1_out), (wo_ref, wo_out))
    copies = []
    for a, (src, dst) in enumerate(weights):
        for p in range(1, n_tp):
            peer = lax.rem(s + p, n_tp)
            copies.append(remote(src.at[peer], dst.at[s], w_send.at[a, p], w_recv.at[a, p], peer, q))
            copies[-1].start()
    local = []
    for a, (src, dst) in enumerate(weights):
        local.append(pltpu.make_async_copy(src.at[s], dst.at[s], loc_sem.at[a]))
        local[-1].start()

    hi, mid, lo = split3(wgt_ref[...])
    parts = jnp.concatenate([hi, mid, lo], axis=0)
    chunk = 1024
    e_iota = lax.broadcasted_iota(jnp.int32, (experts, chunk), 0)
    psum = jnp.zeros((experts, 1), F32)
    count = jnp.zeros((experts, 1), F32)
    for c in range(tokens // chunk):
        cols = pl.ds(c * chunk, chunk)
        lg = dot_nt(parts, x_ref[cols, :])
        logits = lg[:experts] + (lg[experts:2 * experts] + lg[2 * experts:])
        ex = jnp.exp(logits - jnp.max(logits, axis=0, keepdims=True))
        prob = ex / jnp.sum(ex, axis=0, keepdims=True)
        prob_out[:, cols] = prob
        hot1 = e_iota == idx_ref[0:1, cols]
        hot2 = e_iota == idx_ref[1:2, cols]
        g1 = jnp.sum(jnp.where(hot1, prob, 0.0), axis=0, keepdims=True)
        g2 = jnp.sum(jnp.where(hot2, prob, 0.0), axis=0, keepdims=True)
        total = g1 + g2
        gate_out[0:1, cols] = g1 / total
        gate_out[1:2, cols] = g2 / total
        gate_out[2:3, cols] = total
        psum = psum + jnp.sum(prob, axis=1, keepdims=True)
        count = count + jnp.sum(jnp.where(hot1, 1.0, 0.0), axis=1, keepdims=True)
    lane = lax.broadcasted_iota(jnp.int32, (experts, 128), 1)
    stat_buf[...] = jnp.where(lane == 0, count, jnp.where(lane == 1, psum, 0.0))
    for p in range(1, n_ep):
        copies.append(remote(stat_buf, stat_out.at[q], st_send.at[p], st_recv.at[p], s, lax.rem(q + p, n_ep)))
        copies[-1].start()
    local.append(pltpu.make_async_copy(stat_buf, stat_out.at[q], loc_sem.at[3]))
    local[-1].start()

    def row_copies(p, r):
        return (remote(rbuf.at[p], r_out.at[q], row_send.at[0, p], row_recv.at[0, p], s, r),
                remote(dbuf.at[p], d_out.at[q], row_send.at[1, p], row_recv.at[1, p], s, r))

    def own_copies():
        return (pltpu.make_async_copy(rbuf.at[0], r_out.at[q], loc_sem.at[4]),
                pltpu.make_async_copy(dbuf.at[0], d_out.at[q], loc_sem.at[5]))

    tchunk = 512

    def do_dest(i, _):
        p = lax.rem(i + 1, n_ep)
        r = lax.rem(q + p, n_ep)
        base = (r * n_tp + s) * cap
        acc_r[...] = jnp.zeros_like(acc_r)
        acc_d[...] = jnp.zeros_like(acc_d)

        def do_chunk(c, gsum):
            cols = pl.ds(pl.multiple_of(c * tchunk, tchunk), tchunk)
            slot = lax.broadcasted_iota(jnp.int32, (cap, tchunk), 0)
            m1 = (key_ref[0:1, cols] - base) == slot
            m2 = (key_ref[1:2, cols] - base) == slot
            pick = jnp.where(m1 | m2, 1.0, 0.0).astype(BF16)
            acc_r[...] += dot_nn(pick, x_ref[cols, :])
            acc_d[...] += dot_nn(pick, dy_ref[cols, :])
            gsel = jnp.where(m1, gate_out[0:1, cols], 0.0) + jnp.where(m2, gate_out[1:2, cols], 0.0)
            return gsum + jnp.sum(gsel, axis=1, keepdims=True)

        gsum = lax.fori_loop(0, tokens // tchunk, do_chunk, jnp.zeros((cap, 1), F32))
        rbuf[p] = acc_r[...].astype(BF16)
        dbuf[p] = (acc_d[...] * gsum).astype(BF16)

        @pl.when(p > 0)
        def _():
            for cp in row_copies(p, r):
                cp.start()

        @pl.when(p == 0)
        def _():
            for cp in own_copies():
                cp.start()

        return 0

    lax.fori_loop(0, n_ep, do_dest, 0)
    for cp in own_copies():
        cp.wait()
    for cp in local:
        cp.wait()
    for p in range(1, n_ep):
        for cp in row_copies(p, lax.rem(q + p, n_ep)):
            cp.wait()
    for cp in copies:
        cp.wait()


def expert_kernel(n_tp, r_ref, d_ref, w0_ref, w1_ref, wo_ref, rows_out, g0_out, g1_out, go_out,
                  w0c, w1c, h_s, da_s, db_s, acc0, acc1, acco):
    step = pl.program_id(0)
    rows, d_model = r_ref.shape[1], r_ref.shape[2]
    width = wo_ref.shape[0]
    part = width // n_tp

    @pl.when(step == 0)
    def _():
        for j in range(n_tp):
            w0c[:, j * part:(j + 1) * part] = w0_ref[j]
            w1c[:, j * part:(j + 1) * part] = w1_ref[j]
        acc0[...] = jnp.zeros_like(acc0)
        acc1[...] = jnp.zeros_like(acc1)
        acco[...] = jnp.zeros_like(acco)

    r = r_ref[0]
    d = d_ref[0]
    blk = 256
    for j in range(width // blk):
        sl = slice(j * blk, (j + 1) * blk)
        a = dot_nn(r, w0c[:, sl])
        b = dot_nn(r, w1c[:, sl])
        dh = dot_nt(d, wo_ref[sl, :])
        a2 = a * a
        t = jnp.tanh(GELU_C * (a + GELU_A * (a2 * a)))
        cdf = 0.5 * (1.0 + t)
        g = a * cdf
        h_s[:, sl] = (g * b).astype(BF16)
        db_s[:, sl] = (dh * g).astype(BF16)
        slope = cdf + a * (0.5 * (1.0 - t * t) * (GELU_C * (1.0 + (3.0 * GELU_A) * a2)))
        da_s[:, sl] = (dh * b * slope).astype(BF16)
    o = dot_nn(h_s[...], wo_ref[...]).astype(BF16).astype(F32)
    dr = (dot_nt(da_s[...], w0c[...]) + dot_nt(db_s[...], w1c[...])).astype(BF16).astype(F32)
    low = lax.broadcasted_iota(jnp.int32, (rows, 128), 1) < 64
    for j in range(d_model // 128):
        o_blk = o[:, j * 128:(j + 1) * 128]
        r_blk = dr[:, j * 128:(j + 1) * 128]
        rows_out[2 * j, 0] = jnp.where(low, o_blk, pltpu.roll(r_blk, 64, 1)).astype(BF16)
        rows_out[2 * j + 1, 0] = jnp.where(low, pltpu.roll(o_blk, 64, 1), r_blk).astype(BF16)
    acco[...] += dot_tn(h_s[...], d)
    acc0[...] += dot_tn(r, da_s[...])
    acc1[...] += dot_tn(r, db_s[...])

    @pl.when(step == pl.num_programs(0) - 1)
    def _():
        for j in range(n_tp):
            g0_out[j] = acc0[:, j * part:(j + 1) * part].astype(BF16)
            g1_out[j] = acc1[:, j * part:(j + 1) * part].astype(BF16)
        go_out[...] = acco[...].astype(BF16)


def exchange_kernel(n_tp, n_ep, rows_ref, table_out, send, recv, loc):
    s = lax.axis_index("tp")
    q = lax.axis_index("ep")
    me = s * n_ep + q
    copies = []
    for a in range(n_tp):
        for b in range(n_ep):
            if a == 0 and b == 0:
                continue
            tp, ep = lax.rem(s + a, n_tp), lax.rem(q + b, n_ep)
            copies.append(remote(rows_ref.at[tp, ep], table_out.at[me], send.at[a, b], recv.at[a, b], tp, ep))
            copies[-1].start()
    own = pltpu.make_async_copy(rows_ref.at[s, q], table_out.at[me], loc)
    own.start()
    own.wait()
    for cp in copies:
        cp.wait()


def combine_kernel(pos_ref, table_ref, gate_ref, dy_ref, y_out, dr_out, dg_out, tab, c1, c2):
    s = lax.axis_index("tp")
    slots = table_ref.shape[0]
    tokens = dy_ref.shape[0]
    half = tokens // 2
    step = 2048

    def widen(i, _):
        sl = pl.ds(pl.multiple_of(i * step, step), step)
        tab[sl, :] = table_ref[sl, :].astype(F32)
        return 0

    lax.fori_loop(0, slots // step, widen, 0)
    tab[pl.ds(slots, 8), :] = jnp.zeros((8, 128), F32)

    unroll = 16

    def look(i, _):
        t0 = i * unroll
        for u in range(unroll):
            c1[pl.ds(t0 + u, 1), :] = tab[pl.ds(pos_ref[t0 + u], 1), :]
            c2[pl.ds(t0 + u, 1), :] = tab[pl.ds(pos_ref[tokens + t0 + u], 1), :]
        return 0

    lax.fori_loop(0, tokens // unroll, look, 0)

    blk = 512
    low = lax.broadcasted_iota(jnp.int32, (blk, 128), 1) < 64
    odd = lax.rem(s, 2) == 1
    for i in range(half // blk):
        pieces = []
        for h in range(2):
            t0 = h * half + i * blk
            a1 = c1[t0:t0 + blk, :]
            a2 = c2[t0:t0 + blk, :]
            dy = dy_ref[t0:t0 + blk, :].astype(F32)
            dy = jnp.where(odd, pltpu.roll(dy, 64, 1), dy)
            y = gate_ref[t0:t0 + blk, 0:1] * a1 + gate_ref[t0:t0 + blk, 1:2] * a2
            pieces.append((y, a1 + a2))
            for k, av in enumerate((a1, a2)):
                prod = jnp.where(low, dy * av, 0.0)
                line = jnp.sum(prod.T, axis=0, keepdims=True)
                row = k * 4 + t0 // 1024
                col = t0 % 1024
                dg_out[row:row + 1, col:col + blk] = line
        (ya, da), (yb, db) = pieces
        y_out[i * blk:(i + 1) * blk, :] = jnp.where(low, ya, pltpu.roll(yb, 64, 1)).astype(BF16)
        dr_out[i * blk:(i + 1) * blk, :] = jnp.where(low, pltpu.roll(da, 64, 1), db)


def return_kernel(n_tp, n_ep, y_ref, dr_ref, dg_ref, prob_ref, gate_ref, idx_ref, stat_ref, x_ref, wgt_ref,
                  g0_ref, g1_ref, go_ref,
                  gy_out, gx_out, g0_out, g1_out, go_out, dwg_out, aux_out,
                  dg_all, dx_buf, dl_buf, dwg_buf, dwg_all,
                  g_send, g_recv, dg_send, dg_recv, ag_send, ag_recv, wg_send, wg_recv, loc):
    s = lax.axis_index("tp")
    q = lax.axis_index("ep")
    n_z = n_tp // 2
    z = s // 2
    y = lax.rem(s, 2)
    tokens = x_ref.shape[0]
    experts = n_tp * n_ep
    total_tokens = float(tokens * n_ep)
    half = tokens // 2
    copies = []
    for p in range(1, n_tp):
        peer = lax.rem(s + p, n_tp)
        copies.append(remote(dg_ref, dg_all.at[s], dg_send.at[p], dg_recv.at[p], peer, q))
        copies[-1].start()
    dg_copies = list(copies)
    dg_own = pltpu.make_async_copy(dg_ref, dg_all.at[s], loc.at[0])
    dg_own.start()

    class Gather:
        def __init__(self, a, out):
            self.a, self.out = a, out

        def hop(self, src, owner, way, tp):
            return remote(src, self.out.at[owner], ag_send.at[self.a, owner, way], ag_recv.at[self.a, owner], tp, q)

        def up(self, src, owner):
            return self.hop(src, owner, 0, lax.rem(s + 2, n_tp))

        def down(self, src, owner):
            return self.hop(src, owner, 1, lax.rem(s + n_tp - 2, n_tp))

        def across(self, src, owner):
            return self.hop(src, owner, 2, s + 1 - 2 * y)

        def begin(self, src):
            self.src = src
            self.own = pltpu.make_async_copy(src, self.out.at[s], loc.at[1 + self.a])

            @pl.when(z < n_z - 1)
            def _():
                self.up(src, s).start()

            @pl.when(z > 0)
            def _():
                self.down(src, s).start()

            self.across(src, s).start()
            self.own.start()

        def relay(self, dist):
            @pl.when(z >= dist)
            def _():
                owner = lax.rem(s + n_tp - 2 * dist, n_tp)
                blk = self.out.at[owner]
                self.up(blk, owner).wait_recv()

                @pl.when(z < n_z - 1)
                def _():
                    self.up(blk, owner).start()

                self.across(blk, owner).start()

            @pl.when(z + dist < n_z)
            def _():
                owner = lax.rem(s + 2 * dist, n_tp)
                blk = self.out.at[owner]
                self.down(blk, owner).wait_recv()

                @pl.when(z > 0)
                def _():
                    self.down(blk, owner).start()

                self.across(blk, owner).start()

        def finish(self):
            @pl.when(z < n_z - 1)
            def _():
                self.up(self.src, s).wait_send()

            @pl.when(z > 0)
            def _():
                self.down(self.src, s).wait_send()

            self.across(self.src, s).wait_send()
            self.own.wait()
            for dist in range(1, n_z):
                @pl.when(z >= dist)
                def _():
                    owner = lax.rem(s + n_tp - 2 * dist, n_tp)
                    blk = self.out.at[owner]

                    @pl.when(z < n_z - 1)
                    def _():
                        self.up(blk, owner).wait_send()

                    self.across(blk, owner).wait_send()

                @pl.when(z + dist < n_z)
                def _():
                    owner = lax.rem(s + 2 * dist, n_tp)
                    blk = self.out.at[owner]

                    @pl.when(z > 0)
                    def _():
                        self.down(blk, owner).wait_send()

                    self.across(blk, owner).wait_send()

            for k in range(n_z):
                owner = 2 * k + 1 - y
                self.across(self.out.at[owner], owner).wait_recv()

    gat_y = Gather(0, gy_out)
    gat_x = Gather(1, gx_out)
    gat_y.begin(y_ref)

    grads = ((g0_ref, g0_out), (g1_ref, g1_out), (go_ref, go_out))
    local = [dg_own]
    for a, (src, dst) in enumerate(grads):
        for p in range(1, n_tp):
            peer = lax.rem(s + p, n_tp)
            cp = remote(src.at[peer], dst.at[s], g_send.at[a, p], g_recv.at[a, p], peer, q)
            cp.start()
            copies.append(cp)
        local.append(pltpu.make_async_copy(src.at[s], dst.at[s], loc.at[3 + a]))
        local[-1].start()

    counts = stat_ref[0, :, 0:1]
    sums = stat_ref[0, :, 1:2]
    for e in range(1, n_ep):
        counts = counts + stat_ref[e, :, 0:1]
        sums = sums + stat_ref[e, :, 1:2]
    aux_out[...] = jnp.broadcast_to(jnp.sum(counts * sums, axis=0, keepdims=True) * (experts / (total_tokens * total_tokens)), aux_out.shape)
    aux_cot = counts * (AUX_WEIGHT * experts / (total_tokens * total_tokens))
    for cp in dg_copies:
        cp.wait_recv()
    dg_own.wait()
    chunk = 1024
    e_iota = lax.broadcasted_iota(jnp.int32, (experts, chunk), 0)
    for c in range(tokens // chunk):
        cols = pl.ds(c * chunk, chunk)
        dw1 = dg_all[0, c:c + 1, :]
        dw2 = dg_all[0, 4 + c:5 + c, :]
        for o in range(1, n_tp):
            dw1 = dw1 + dg_all[o, c:c + 1, :]
            dw2 = dw2 + dg_all[o, 4 + c:5 + c, :]
        w1 = gate_ref[0:1, cols]
        w2 = gate_ref[1:2, cols]
        tot = gate_ref[2:3, cols]
        mean = dw1 * w1 + dw2 * w2
        dg1 = (dw1 - mean) / tot
        dg2 = (dw2 - mean) / tot
        prob = prob_ref[:, cols]
        dp = jnp.where(e_iota == idx_ref[0:1, cols], dg1, 0.0) + jnp.where(e_iota == idx_ref[1:2, cols], dg2, 0.0) + aux_cot
        dl = prob * (dp - jnp.sum(prob * dp, axis=0, keepdims=True))
        hi, mid, lo = split3(dl)
        dl_buf[0:experts, cols] = hi
        dl_buf[experts:2 * experts, cols] = mid
        dl_buf[2 * experts:, cols] = lo

    whi, wmid, wlo = split3(wgt_ref[...])
    left = lax.broadcasted_iota(jnp.int32, (half, 128), 1) < 64
    w_top = jnp.concatenate([whi, whi, whi], axis=0)
    w_mid = jnp.concatenate([wmid, wmid], axis=0)
    dl_all = dl_buf[...]
    xr = dot_tn(dl_all, w_top) + dot_tn(dl_all[:2 * experts], w_mid) + dot_tn(dl_all[:experts], wlo)
    xr = jnp.where(left, xr[:half], pltpu.roll(xr[half:], 64, 1))
    dx_buf[...] = (dr_ref[...] + xr).astype(BF16)
    gat_x.begin(dx_buf)
    gat_y.relay(1)
    dw = dot_nn(dl_all, x_ref[...])
    dwg_buf[...] = dw[:experts] + (dw[experts:2 * experts] + dw[2 * experts:])
    wg_copies = []
    for p in range(1, n_ep):
        cp = remote(dwg_buf, dwg_all.at[q], wg_send.at[p], wg_recv.at[p], s, lax.rem(q + p, n_ep))
        cp.start()
        wg_copies.append(cp)
    wg_own = pltpu.make_async_copy(dwg_buf, dwg_all.at[q], loc.at[6])
    wg_own.start()
    gat_y.relay(2)
    gat_x.relay(1)
    gat_y.relay(3)
    gat_x.relay(2)
    gat_x.relay(3)
    wg_own.wait()
    for cp in wg_copies:
        cp.wait()
    tot = dwg_all[0]
    for e in range(1, n_ep):
        tot = tot + dwg_all[e]
    dwg_out[...] = tot
    gat_y.finish()
    gat_x.finish()
    for cp in dg_copies:
        cp.wait_send()
    for cp in local[1:]:
        cp.wait()
    for cp in copies[len(dg_copies):]:
        cp.wait()


def interleave_kernel(gy_ref, gx_ref, y_out, dx_out):
    half = gy_ref.shape[1]
    low = lax.broadcasted_iota(jnp.int32, (half, 128), 1) < 64
    for src, dst in ((gy_ref, y_out), (gx_ref, dx_out)):
        a = src[0].astype(F32)
        b = src[1].astype(F32)
        dst[0:half, :] = jnp.where(low, a, pltpu.roll(b, 64, 1)).astype(BF16)
        dst[half:2 * half, :] = jnp.where(low, pltpu.roll(a, 64, 1), b).astype(BF16)


def solution(mesh):
    n_ep = mesh.shape["ep"]
    n_tp = mesh.shape["tp"]
    vmem = pl.BlockSpec(memory_space=pltpu.VMEM)
    hbm = pl.BlockSpec(memory_space=ANY)
    dma = pltpu.SemaphoreType.DMA
    sds = jax.ShapeDtypeStruct

    def device_step(x_loc, w_router, idx_loc, slot_loc, gelu_loc, lin_loc, out_loc, dy_loc):
        tokens, d_model = x_loc.shape
        exp_local = gelu_loc.shape[0]
        part = gelu_loc.shape[2]
        width = part * n_tp
        experts = exp_local * n_ep
        cap = 4 * tokens // experts
        slots = experts * cap
        s = lax.axis_index("tp")
        idx_t = idx_loc.T
        slot_t = slot_loc.T
        kept = slot_t < cap
        key_t = jnp.where(kept, idx_t * cap + slot_t, -1)
        pos = jnp.where(kept, ((idx_t % n_tp) * n_ep + idx_t // n_tp) * cap + slot_t, slots).reshape(-1)
        wgt = w_router.T
        side = pltpu.CompilerParams(has_side_effects=True, vmem_limit_bytes=VMEM_LIMIT)

        rows, drows, w0, w1, wo, prob, gate, stat = pl.pallas_call(
            functools.partial(dispatch_kernel, n_tp, n_ep, cap),
            name="moe_dispatch",
            out_shape=(sds((n_ep, cap, d_model), BF16), sds((n_ep, cap, d_model), BF16),
                       sds(gelu_loc.shape, BF16), sds(lin_loc.shape, BF16), sds(out_loc.shape, BF16),
                       sds((experts, tokens), F32), sds((8, tokens), F32), sds((n_ep, experts, 128), F32)),
            in_specs=[vmem] * 5 + [hbm] * 3,
            out_specs=(hbm, hbm, hbm, hbm, hbm, vmem, vmem, vmem),
            scratch_shapes=[pltpu.VMEM((n_ep, cap, d_model), BF16), pltpu.VMEM((n_ep, cap, d_model), BF16),
                            pltpu.VMEM((experts, 128), F32), pltpu.VMEM((cap, d_model), F32), pltpu.VMEM((cap, d_model), F32),
                            dma((3, n_tp)), dma((3, n_tp)), dma((2, n_ep)), dma((2, n_ep)), dma((n_ep,)), dma((n_ep,)), dma((6,))],
            compiler_params=side,
        )(x_loc, dy_loc, idx_t, key_t, wgt, gelu_loc, lin_loc, out_loc)

        full = lambda shape: pl.BlockSpec(shape, lambda i: (0,) * len(shape))
        back, g0, g1, go = pl.pallas_call(
            functools.partial(expert_kernel, n_tp),
            name="moe_expert",
            grid=(n_ep,),
            out_shape=(sds((n_tp, n_ep, cap, 128), BF16), sds((n_tp, d_model, part), BF16), sds((n_tp, d_model, part), BF16), sds((width, d_model), BF16)),
            in_specs=[pl.BlockSpec((1, cap, d_model), lambda i: (i, 0, 0)), pl.BlockSpec((1, cap, d_model), lambda i: (i, 0, 0)),
                      full((n_tp, d_model, part)), full((n_tp, d_model, part)), full((width, d_model))],
            out_specs=(pl.BlockSpec((n_tp, 1, cap, 128), lambda i: (0, i, 0, 0)), full((n_tp, d_model, part)), full((n_tp, d_model, part)), full((width, d_model))),
            scratch_shapes=[pltpu.VMEM((d_model, width), BF16), pltpu.VMEM((d_model, width), BF16),
                            pltpu.VMEM((cap, width), BF16), pltpu.VMEM((cap, width), BF16), pltpu.VMEM((cap, width), BF16),
                            pltpu.VMEM((d_model, width), F32), pltpu.VMEM((d_model, width), F32), pltpu.VMEM((width, d_model), F32)],
            compiler_params=pltpu.CompilerParams(dimension_semantics=("arbitrary",), vmem_limit_bytes=VMEM_LIMIT),
        )(rows, drows, w0, w1, wo.reshape(width, d_model))

        table = pl.pallas_call(
            functools.partial(exchange_kernel, n_tp, n_ep),
            name="moe_exchange",
            out_shape=sds((n_tp * n_ep, cap, 128), BF16),
            in_specs=[hbm],
            out_specs=hbm,
            scratch_shapes=[dma((n_tp, n_ep)), dma((n_tp, n_ep)), dma(())],
            compiler_params=side,
        )(back)

        dy_cols = lax.dynamic_slice_in_dim(dy_loc, (s // 2) * 128, 128, axis=1)
        y_pk, dr_pk, dg = pl.pallas_call(
            combine_kernel,
            name="moe_combine",
            out_shape=(sds((tokens // 2, 128), BF16), sds((tokens // 2, 128), F32), sds((8, tokens // 4), F32)),
            in_specs=[pl.BlockSpec(memory_space=pltpu.SMEM), vmem, vmem, vmem],
            out_specs=(vmem, vmem, vmem),
            scratch_shapes=[pltpu.VMEM((slots + 8, 128), F32), pltpu.VMEM((tokens, 128), F32), pltpu.VMEM((tokens, 128), F32)],
            compiler_params=pltpu.CompilerParams(vmem_limit_bytes=VMEM_LIMIT),
        )(pos, table.reshape(slots, 128), gate[:2].T, dy_cols)

        col0 = s * (d_model // n_tp)
        wg_cols = jnp.pad(lax.dynamic_slice_in_dim(wgt, col0, d_model // n_tp, axis=1), ((0, 0), (0, 64)))
        gy, gx, grad_gelu, grad_lin, grad_out, dwg_t, aux = pl.pallas_call(
            functools.partial(return_kernel, n_tp, n_ep),
            name="moe_return",
            out_shape=(sds((n_tp, tokens // 2, 128), BF16), sds((n_tp, tokens // 2, 128), BF16),
                       sds(gelu_loc.shape, BF16), sds(lin_loc.shape, BF16), sds(out_loc.shape, BF16),
                       sds((experts, d_model), F32), sds((8, 128), F32)),
            in_specs=[vmem] * 9 + [hbm] * 3,
            out_specs=(hbm, hbm, hbm, hbm, hbm, vmem, vmem),
            scratch_shapes=[pltpu.VMEM((n_tp, 8, tokens // 4), F32), pltpu.VMEM((tokens // 2, 128), BF16),
                            pltpu.VMEM((3 * experts, tokens), BF16), pltpu.VMEM((experts, d_model), F32), pltpu.VMEM((n_ep, experts, d_model), F32),
                            dma((3, n_tp)), dma((3, n_tp)), dma((n_tp,)), dma((n_tp,)),
                            dma((2, n_tp, 3)), dma((2, n_tp)), dma((n_ep,)), dma((n_ep,)), dma((7,))],
            compiler_params=side,
        )(y_pk, dr_pk, dg, prob, gate, idx_t, stat, x_loc, wg_cols, g0, g1, go.reshape(out_loc.shape))

        pair = pl.BlockSpec((2, tokens // 2, 128), lambda j: (j, 0, 0))
        cols = pl.BlockSpec((tokens, 128), lambda j: (0, j))
        y_loc, dx_loc = pl.pallas_call(
            interleave_kernel,
            name="moe_interleave",
            grid=(n_tp // 2,),
            out_shape=(sds((tokens, d_model), BF16), sds((tokens, d_model), BF16)),
            in_specs=[pair, pair],
            out_specs=(cols, cols),
            compiler_params=pltpu.CompilerParams(dimension_semantics=("arbitrary",), vmem_limit_bytes=VMEM_LIMIT),
        )(gy, gx)
        return y_loc, dx_loc, grad_gelu, grad_lin, grad_out, dwg_t.T, aux[0, 0]

    rows_spec = P("ep", None)
    weight_in = P("ep", None, "tp")
    weight_out = P("ep", "tp", None)
    return jax.shard_map(
        device_step,
        mesh=mesh,
        in_specs=(rows_spec, P(None, None), rows_spec, rows_spec, weight_in, weight_in, weight_out, rows_spec),
        out_specs=(rows_spec, rows_spec, weight_in, weight_in, weight_out, P(None, None), P()),
        check_vma=False,
    )
```

```python
import functools

import jax
import jax.numpy as jnp
from jax import lax
from jax.experimental import pallas as pl
from jax.experimental.pallas import tpu as pltpu
from jax.sharding import PartitionSpec as P

AUX_WEIGHT = 0.01
F32 = jnp.float32
BF16 = jnp.bfloat16
VMEM_LIMIT = 64000 * 1024
GELU_C = 0.7978845608028654
GELU_A = 0.044715
ANY = pl.ANY


def dot_nn(a, b):
    return lax.dot_general(a, b, (((1,), (0,)), ((), ())), preferred_element_type=F32)


def dot_nt(a, b):
    return lax.dot_general(a, b, (((1,), (1,)), ((), ())), preferred_element_type=F32)


def dot_tn(a, b):
    return lax.dot_general(a, b, (((0,), (0,)), ((), ())), preferred_element_type=F32)


def split3(v):
    hi = v.astype(BF16)
    rest = v - hi.astype(F32)
    mid = rest.astype(BF16)
    lo = (rest - mid.astype(F32)).astype(BF16)
    return hi, mid, lo


def remote(src, dst, send_sem, recv_sem, tp, ep):
    return pltpu.make_async_remote_copy(
        src_ref=src, dst_ref=dst, send_sem=send_sem, recv_sem=recv_sem,
        device_id={"tp": tp, "ep": ep}, device_id_type=pl.DeviceIdType.MESH,
    )


def dispatch_kernel(n_tp, n_ep, cap, x_ref, dy_ref, idx_ref, key_ref, wgt_ref, w0_ref, w1_ref, wo_ref,
                    r_out, d_out, w0_out, w1_out, wo_out, prob_out, gate_out, stat_out, dyc_out, gcol_out,
                    x_buf, dy_buf, rbuf, dbuf, stat_buf, acc_r, acc_d, w_send, w_recv, row_send, row_recv, st_send, st_recv, loc_sem):
    s = lax.axis_index("tp")
    q = lax.axis_index("ep")
    tokens = x_ref.shape[0]
    experts = n_tp * n_ep
    weights = ((w0_ref, w0_out), (w1_ref, w1_out), (wo_ref, wo_out))
    copies = []
    for a, (src, dst) in enumerate(weights):
        for p in range(1, n_tp):
            peer = lax.rem(s + p, n_tp)
            copies.append(remote(src.at[peer], dst.at[s], w_send.at[a, p], w_recv.at[a, p], peer, q))
            copies[-1].start()
    x_load = pltpu.make_async_copy(x_ref, x_buf, loc_sem.at[6])
    dy_load = pltpu.make_async_copy(dy_ref, dy_buf, loc_sem.at[7])
    x_load.start()
    dy_load.start()
    local = []
    for a, (src, dst) in enumerate(weights):
        local.append(pltpu.make_async_copy(src.at[s], dst.at[s], loc_sem.at[a]))
        local[-1].start()

    hi, mid, lo = split3(wgt_ref[...])
    parts = jnp.concatenate([hi, mid, lo], axis=0)
    chunk = 1024
    e_iota = lax.broadcasted_iota(jnp.int32, (experts, chunk), 0)
    psum = jnp.zeros((experts, 1), F32)
    count = jnp.zeros((experts, 1), F32)
    x_load.wait()
    for c in range(tokens // chunk):
        cols = pl.ds(c * chunk, chunk)
        lg = dot_nt(parts, x_buf[cols, :])
        logits = lg[:experts] + (lg[experts:2 * experts] + lg[2 * experts:])
        ex = jnp.exp(logits - jnp.max(logits, axis=0, keepdims=True))
        prob = ex / jnp.sum(ex, axis=0, keepdims=True)
        prob_out[:, cols] = prob
        hot1 = e_iota == idx_ref[0:1, cols]
        hot2 = e_iota == idx_ref[1:2, cols]
        g1 = jnp.sum(jnp.where(hot1, prob, 0.0), axis=0, keepdims=True)
        g2 = jnp.sum(jnp.where(hot2, prob, 0.0), axis=0, keepdims=True)
        total = g1 + g2
        gate_out[0:1, cols] = g1 / total
        gate_out[1:2, cols] = g2 / total
        gate_out[2:3, cols] = total
        gate_out[3:8, cols] = jnp.zeros((5, chunk), F32)
        psum = psum + jnp.sum(prob, axis=1, keepdims=True)
        count = count + jnp.sum(jnp.where(hot1, 1.0, 0.0), axis=1, keepdims=True)
    lane = lax.broadcasted_iota(jnp.int32, (experts, 128), 1)
    stat_buf[...] = jnp.where(lane == 0, count, jnp.where(lane == 1, psum, 0.0))
    for p in range(1, n_ep):
        copies.append(remote(stat_buf, stat_out.at[q], st_send.at[p], st_recv.at[p], s, lax.rem(q + p, n_ep)))
        copies[-1].start()
    local.append(pltpu.make_async_copy(stat_buf, stat_out.at[q], loc_sem.at[3]))
    local[-1].start()

    def row_copies(p, r):
        return (remote(rbuf.at[p], r_out.at[q], row_send.at[0, p], row_recv.at[0, p], s, r),
                remote(dbuf.at[p], d_out.at[q], row_send.at[1, p], row_recv.at[1, p], s, r))

    def own_copies():
        return (pltpu.make_async_copy(rbuf.at[0], r_out.at[q], loc_sem.at[4]),
                pltpu.make_async_copy(dbuf.at[0], d_out.at[q], loc_sem.at[5]))

    tchunk = 512
    dy_load.wait()

    def do_dest(i, _):
        p = lax.rem(i + 1, n_ep)
        r = lax.rem(q + p, n_ep)
        base = (r * n_tp + s) * cap
        acc_r[...] = jnp.zeros_like(acc_r)
        acc_d[...] = jnp.zeros_like(acc_d)

        def do_chunk(c, gsum):
            cols = pl.ds(pl.multiple_of(c * tchunk, tchunk), tchunk)
            slot = lax.broadcasted_iota(jnp.int32, (cap, tchunk), 0)
            m1 = (key_ref[0:1, cols] - base) == slot
            m2 = (key_ref[1:2, cols] - base) == slot
            pick = jnp.where(m1 | m2, 1.0, 0.0).astype(BF16)
            acc_r[...] += dot_nn(pick, x_buf[cols, :])
            acc_d[...] += dot_nn(pick, dy_buf[cols, :])
            gsel = jnp.where(m1, gate_out[0:1, cols], 0.0) + jnp.where(m2, gate_out[1:2, cols], 0.0)
            return gsum + jnp.sum(gsel, axis=1, keepdims=True)

        gsum = lax.fori_loop(0, tokens // tchunk, do_chunk, jnp.zeros((cap, 1), F32))
        rbuf[p] = acc_r[...].astype(BF16)
        dbuf[p] = (acc_d[...] * gsum).astype(BF16)

        @pl.when(p > 0)
        def _():
            for cp in row_copies(p, r):
                cp.start()

        @pl.when(p == 0)
        def _():
            for cp in own_copies():
                cp.start()

        return 0

    lax.fori_loop(0, n_ep, do_dest, 0)

    pair = pl.ds(pl.multiple_of((s // 2) * 128, 128), 128)
    odd = lax.rem(s, 2) == 1
    for c in range(tokens // chunk):
        cols = pl.ds(c * chunk, chunk)
        dyc = dy_buf[cols, pair].astype(F32)
        dyc_out[cols, :] = jnp.where(odd, pltpu.roll(dyc, 64, 1), dyc).astype(BF16)
        gcol_out[cols, :] = gate_out[:, cols].T
    for cp in own_copies():
        cp.wait()
    for cp in local:
        cp.wait()
    for p in range(1, n_ep):
        for cp in row_copies(p, lax.rem(q + p, n_ep)):
            cp.wait()
    for cp in copies:
        cp.wait()


def expert_kernel(n_tp, n_ep, r_ref, d_ref, w0_ref, w1_ref, wo_ref, table_out, g0_out, g1_out, go_out,
                  w0c, w1c, h_s, da_s, db_s, acc0, acc1, acco, back, send, recv, loc):
    s = lax.axis_index("tp")
    q = lax.axis_index("ep")
    me = s * n_ep + q
    rows, d_model = r_ref.shape[1], r_ref.shape[2]
    width = wo_ref.shape[0]
    part = width // n_tp
    for j in range(n_tp):
        w0c[:, j * part:(j + 1) * part] = w0_ref[j]
        w1c[:, j * part:(j + 1) * part] = w1_ref[j]
    acc0[...] = jnp.zeros_like(acc0)
    acc1[...] = jnp.zeros_like(acc1)
    acco[...] = jnp.zeros_like(acco)

    def row_copy(a, b):
        tp, ep = lax.rem(s + a, n_tp), lax.rem(q + b, n_ep)
        return remote(back.at[tp, ep], table_out.at[me], send.at[a, b], recv.at[a, b], tp, ep)

    own = pltpu.make_async_copy(back.at[s, q], table_out.at[me], loc)

    def shard(i, _):
        b = lax.rem(i + 1, n_ep)
        ep = lax.rem(q + b, n_ep)
        r = r_ref[ep]
        d = d_ref[ep]
        blk = 256
        for j in range(width // blk):
            sl = slice(j * blk, (j + 1) * blk)
            u = dot_nn(r, w0c[:, sl])
            v = dot_nn(r, w1c[:, sl])
            dh = dot_nt(d, wo_ref[sl, :])
            u2 = u * u
            t = jnp.tanh(GELU_C * (u + GELU_A * (u2 * u)))
            cdf = 0.5 * (1.0 + t)
            g = u * cdf
            h_s[:, sl] = (g * v).astype(BF16)
            db_s[:, sl] = (dh * g).astype(BF16)
            slope = cdf + u * (0.5 * (1.0 - t * t) * (GELU_C * (1.0 + (3.0 * GELU_A) * u2)))
            da_s[:, sl] = (dh * v * slope).astype(BF16)
        o = dot_nn(h_s[...], wo_ref[...]).astype(BF16).astype(F32)
        dr = (dot_nt(da_s[...], w0c[...]) + dot_nt(db_s[...], w1c[...])).astype(BF16).astype(F32)
        low = lax.broadcasted_iota(jnp.int32, (rows, 128), 1) < 64
        for j in range(d_model // 128):
            o_blk = o[:, j * 128:(j + 1) * 128]
            r_blk = dr[:, j * 128:(j + 1) * 128]
            back[2 * j, ep] = jnp.where(low, o_blk, pltpu.roll(r_blk, 64, 1)).astype(BF16)
            back[2 * j + 1, ep] = jnp.where(low, pltpu.roll(o_blk, 64, 1), r_blk).astype(BF16)
        for a in range(1, n_tp):
            row_copy(a, b).start()

        @pl.when(b > 0)
        def _():
            row_copy(0, b).start()

        @pl.when(b == 0)
        def _():
            own.start()

        acco[...] += dot_tn(h_s[...], d)
        acc0[...] += dot_tn(r, da_s[...])
        acc1[...] += dot_tn(r, db_s[...])
        return 0

    lax.fori_loop(0, n_ep, shard, 0)
    for j in range(n_tp):
        g0_out[j] = acc0[:, j * part:(j + 1) * part].astype(BF16)
        g1_out[j] = acc1[:, j * part:(j + 1) * part].astype(BF16)
    go_out[...] = acco[...].astype(BF16)
    own.wait()
    for b in range(n_ep):
        for a in range(n_tp):
            if a + b > 0:
                row_copy(a, b).wait()


def return_kernel(n_tp, n_ep, pos_ref, gcol_ref, dyc_ref, prob_ref, gate_ref, idx_ref, stat_ref, wgt_ref,
                  table_ref, x_ref, g0_ref, g1_ref, go_ref,
                  gy_out, gx_out, g0_out, g1_out, go_out, dwg_out, aux_out,
                  tab_in, tab, c1, c2, y_buf, dr_buf, dg_buf, x_buf, tab_sem,
                  dg_all, dx_buf, dl_buf, dwg_buf, dwg_all,
                  g_send, g_recv, dg_send, dg_recv, ag_send, ag_recv, wg_send, wg_recv, loc):
    s = lax.axis_index("tp")
    q = lax.axis_index("ep")
    n_z = n_tp // 2
    z = s // 2
    y = lax.rem(s, 2)
    tokens = x_ref.shape[0]
    experts = n_tp * n_ep
    total_tokens = float(tokens * n_ep)
    half = tokens // 2
    copies = []
    local = []
    grads = ((g0_ref, g0_out), (g1_ref, g1_out), (go_ref, go_out))

    def send_grads(a):
        src, dst = grads[a]
        for p in range(1, n_tp):
            peer = lax.rem(s + p, n_tp)
            cp = remote(src.at[peer], dst.at[s], g_send.at[a, p], g_recv.at[a, p], peer, q)
            cp.start()
            copies.append(cp)
        local.append(pltpu.make_async_copy(src.at[s], dst.at[s], loc.at[3 + a]))
        local[-1].start()

    class Gather:
        def __init__(self, a, out):
            self.a, self.out = a, out

        def hop(self, src, owner, way, tp):
            return remote(src, self.out.at[owner], ag_send.at[self.a, owner, way], ag_recv.at[self.a, owner], tp, q)

        def up(self, src, owner):
            return self.hop(src, owner, 0, lax.rem(s + 2, n_tp))

        def down(self, src, owner):
            return self.hop(src, owner, 1, lax.rem(s + n_tp - 2, n_tp))

        def across(self, src, owner):
            return self.hop(src, owner, 2, s + 1 - 2 * y)

        def begin(self, src):
            self.src = src
            self.own = pltpu.make_async_copy(src, self.out.at[s], loc.at[1 + self.a])

            @pl.when(z < n_z - 1)
            def _():
                self.up(src, s).start()

            @pl.when(z > 0)
            def _():
                self.down(src, s).start()

            self.across(src, s).start()
            self.own.start()

        def relay(self, dist):
            @pl.when(z >= dist)
            def _():
                owner = lax.rem(s + n_tp - 2 * dist, n_tp)
                blk = self.out.at[owner]
                self.up(blk, owner).wait_recv()

                @pl.when(z < n_z - 1)
                def _():
                    self.up(blk, owner).start()

                self.across(blk, owner).start()

            @pl.when(z + dist < n_z)
            def _():
                owner = lax.rem(s + 2 * dist, n_tp)
                blk = self.out.at[owner]
                self.down(blk, owner).wait_recv()

                @pl.when(z > 0)
                def _():
                    self.down(blk, owner).start()

                self.across(blk, owner).start()

        def finish(self):
            @pl.when(z < n_z - 1)
            def _():
                self.up(self.src, s).wait_send()

            @pl.when(z > 0)
            def _():
                self.down(self.src, s).wait_send()

            self.across(self.src, s).wait_send()
            self.own.wait()
            for dist in range(1, n_z):
                @pl.when(z >= dist)
                def _():
                    owner = lax.rem(s + n_tp - 2 * dist, n_tp)
                    blk = self.out.at[owner]

                    @pl.when(z < n_z - 1)
                    def _():
                        self.up(blk, owner).wait_send()

                    self.across(blk, owner).wait_send()

                @pl.when(z + dist < n_z)
                def _():
                    owner = lax.rem(s + 2 * dist, n_tp)
                    blk = self.out.at[owner]

                    @pl.when(z > 0)
                    def _():
                        self.down(blk, owner).wait_send()

                    self.across(blk, owner).wait_send()

            for k in range(n_z):
                owner = 2 * k + 1 - y
                self.across(self.out.at[owner], owner).wait_recv()

    gat_y = Gather(0, gy_out)
    gat_x = Gather(1, gx_out)
    slots = tab_in.shape[0] * tab_in.shape[1]
    cap = tab_in.shape[1]
    groups = 8
    per = tab_in.shape[0] // groups
    loads = [pltpu.make_async_copy(table_ref.at[pl.ds(k * per, per)], tab_in.at[pl.ds(k * per, per)], tab_sem.at[k]) for k in range(groups)]
    for cp in loads:
        cp.start()
    x_load = pltpu.make_async_copy(x_ref, x_buf, loc.at[7])
    x_load.start()
    send_grads(0)

    tab[pl.ds(slots, 8), :] = jnp.zeros((8, 128), F32)
    for k in range(groups):
        loads[k].wait()

        def widen(i, _):
            tab[pl.ds(pl.multiple_of((k * per + i) * cap, cap), cap), :] = tab_in[k * per + i].astype(F32)
            return 0

        lax.fori_loop(0, per, widen, 0)

    unroll = 16

    def look(i, _):
        t0 = i * unroll
        for u in range(unroll):
            c1[pl.ds(t0 + u, 1), :] = tab[pl.ds(pos_ref[t0 + u], 1), :]
            c2[pl.ds(t0 + u, 1), :] = tab[pl.ds(pos_ref[tokens + t0 + u], 1), :]
        return 0

    lax.fori_loop(0, tokens // unroll, look, 0)

    blk = 512
    low = lax.broadcasted_iota(jnp.int32, (blk, 128), 1) < 64
    for i in range(half // blk):
        pieces = []
        for h in range(2):
            t0 = h * half + i * blk
            a1 = c1[t0:t0 + blk, :]
            a2 = c2[t0:t0 + blk, :]
            dy = dyc_ref[t0:t0 + blk, :].astype(F32)
            pieces.append((gcol_ref[t0:t0 + blk, 0:1] * a1 + gcol_ref[t0:t0 + blk, 1:2] * a2, a1 + a2))
            for k, av in enumerate((a1, a2)):
                prod = jnp.where(low, dy * av, 0.0)
                row = k * 4 + t0 // 1024
                col = t0 % 1024
                dg_buf[row:row + 1, col:col + blk] = jnp.sum(prod.T, axis=0, keepdims=True)
        (ya, da), (yb, db) = pieces
        y_buf[i * blk:(i + 1) * blk, :] = jnp.where(low, ya, pltpu.roll(yb, 64, 1)).astype(BF16)
        dr_buf[i * blk:(i + 1) * blk, :] = jnp.where(low, pltpu.roll(da, 64, 1), db)

    dg_copies = []
    for p in range(1, n_tp):
        peer = lax.rem(s + p, n_tp)
        dg_copies.append(remote(dg_buf, dg_all.at[s], dg_send.at[p], dg_recv.at[p], peer, q))
        dg_copies[-1].start()
    dg_own = pltpu.make_async_copy(dg_buf, dg_all.at[s], loc.at[0])
    dg_own.start()
    gat_y.begin(y_buf)

    counts = stat_ref[0, :, 0:1]
    sums = stat_ref[0, :, 1:2]
    for e in range(1, n_ep):
        counts = counts + stat_ref[e, :, 0:1]
        sums = sums + stat_ref[e, :, 1:2]
    aux_out[...] = jnp.broadcast_to(jnp.sum(counts * sums, axis=0, keepdims=True) * (experts / (total_tokens * total_tokens)), aux_out.shape)
    aux_cot = counts * (AUX_WEIGHT * experts / (total_tokens * total_tokens))
    for cp in dg_copies:
        cp.wait_recv()
    dg_own.wait()
    chunk = 1024
    e_iota = lax.broadcasted_iota(jnp.int32, (experts, chunk), 0)
    for c in range(tokens // chunk):
        cols = pl.ds(c * chunk, chunk)
        dw1 = dg_all[0, c:c + 1, :]
        dw2 = dg_all[0, 4 + c:5 + c, :]
        for o in range(1, n_tp):
            dw1 = dw1 + dg_all[o, c:c + 1, :]
            dw2 = dw2 + dg_all[o, 4 + c:5 + c, :]
        w1 = gate_ref[0:1, cols]
        w2 = gate_ref[1:2, cols]
        tot = gate_ref[2:3, cols]
        mean = dw1 * w1 + dw2 * w2
        dg1 = (dw1 - mean) / tot
        dg2 = (dw2 - mean) / tot
        prob = prob_ref[:, cols]
        dp = jnp.where(e_iota == idx_ref[0:1, cols], dg1, 0.0) + jnp.where(e_iota == idx_ref[1:2, cols], dg2, 0.0) + aux_cot
        dl = prob * (dp - jnp.sum(prob * dp, axis=0, keepdims=True))
        hi, mid, lo = split3(dl)
        dl_buf[0:experts, cols] = hi
        dl_buf[experts:2 * experts, cols] = mid
        dl_buf[2 * experts:, cols] = lo

    whi, wmid, wlo = split3(wgt_ref[...])
    left = lax.broadcasted_iota(jnp.int32, (half, 128), 1) < 64
    w_top = jnp.concatenate([whi, whi, whi], axis=0)
    w_mid = jnp.concatenate([wmid, wmid], axis=0)
    dl_all = dl_buf[...]
    xr = dot_tn(dl_all, w_top) + dot_tn(dl_all[:2 * experts], w_mid) + dot_tn(dl_all[:experts], wlo)
    xr = jnp.where(left, xr[:half], pltpu.roll(xr[half:], 64, 1))
    dx_buf[...] = (dr_buf[...] + xr).astype(BF16)
    gat_x.begin(dx_buf)
    gat_y.relay(1)
    x_load.wait()
    dw = dot_nn(dl_all, x_buf[...])
    dwg_buf[...] = dw[:experts] + (dw[experts:2 * experts] + dw[2 * experts:])
    wg_copies = []
    for p in range(1, n_ep):
        cp = remote(dwg_buf, dwg_all.at[q], wg_send.at[p], wg_recv.at[p], s, lax.rem(q + p, n_ep))
        cp.start()
        wg_copies.append(cp)
    wg_own = pltpu.make_async_copy(dwg_buf, dwg_all.at[q], loc.at[6])
    wg_own.start()
    gat_y.relay(2)
    gat_x.relay(1)
    send_grads(1)
    gat_y.relay(3)
    gat_x.relay(2)
    send_grads(2)
    gat_x.relay(3)
    wg_own.wait()
    for cp in wg_copies:
        cp.wait()
    tot = dwg_all[0]
    for e in range(1, n_ep):
        tot = tot + dwg_all[e]
    dwg_out[...] = tot
    gat_y.finish()
    gat_x.finish()
    for cp in dg_copies:
        cp.wait_send()
    for cp in local:
        cp.wait()
    for cp in copies:
        cp.wait()


def interleave_kernel(gy_ref, gx_ref, y_out, dx_out):
    half = gy_ref.shape[1]
    low = lax.broadcasted_iota(jnp.int32, (half, 128), 1) < 64
    for src, dst in ((gy_ref, y_out), (gx_ref, dx_out)):
        a = src[0].astype(F32)
        b = src[1].astype(F32)
        dst[0:half, :] = jnp.where(low, a, pltpu.roll(b, 64, 1)).astype(BF16)
        dst[half:2 * half, :] = jnp.where(low, pltpu.roll(a, 64, 1), b).astype(BF16)


def solution(mesh):
    n_ep = mesh.shape["ep"]
    n_tp = mesh.shape["tp"]
    vmem = pl.BlockSpec(memory_space=pltpu.VMEM)
    hbm = pl.BlockSpec(memory_space=ANY)
    dma = pltpu.SemaphoreType.DMA
    sds = jax.ShapeDtypeStruct

    def device_step(x_loc, w_router, idx_loc, slot_loc, gelu_loc, lin_loc, out_loc, dy_loc):
        tokens, d_model = x_loc.shape
        exp_local = gelu_loc.shape[0]
        part = gelu_loc.shape[2]
        width = part * n_tp
        experts = exp_local * n_ep
        cap = 4 * tokens // experts
        slots = experts * cap
        s = lax.axis_index("tp")
        idx_t = idx_loc.T
        slot_t = slot_loc.T
        kept = slot_t < cap
        key_t = jnp.where(kept, idx_t * cap + slot_t, -1)
        pos = jnp.where(kept, ((idx_t % n_tp) * n_ep + idx_t // n_tp) * cap + slot_t, slots).reshape(-1)
        wgt = w_router.T
        side = pltpu.CompilerParams(has_side_effects=True, vmem_limit_bytes=VMEM_LIMIT)

        rows, drows, w0, w1, wo, prob, gate, stat, dy_cols, gate_cols = pl.pallas_call(
            functools.partial(dispatch_kernel, n_tp, n_ep, cap),
            name="moe_dispatch",
            out_shape=(sds((n_ep, cap, d_model), BF16), sds((n_ep, cap, d_model), BF16),
                       sds(gelu_loc.shape, BF16), sds(lin_loc.shape, BF16), sds(out_loc.shape, BF16),
                       sds((experts, tokens), F32), sds((8, tokens), F32), sds((n_ep, experts, 128), F32),
                       sds((tokens, 128), BF16), sds((tokens, 8), F32)),
            in_specs=[hbm] * 2 + [vmem] * 3 + [hbm] * 3,
            out_specs=(hbm, hbm, hbm, hbm, hbm, vmem, vmem, vmem, vmem, vmem),
            scratch_shapes=[pltpu.VMEM((tokens, d_model), BF16), pltpu.VMEM((tokens, d_model), BF16),
                            pltpu.VMEM((n_ep, cap, d_model), BF16), pltpu.VMEM((n_ep, cap, d_model), BF16),
                            pltpu.VMEM((experts, 128), F32), pltpu.VMEM((cap, d_model), F32), pltpu.VMEM((cap, d_model), F32),
                            dma((3, n_tp)), dma((3, n_tp)), dma((2, n_ep)), dma((2, n_ep)), dma((n_ep,)), dma((n_ep,)), dma((8,))],
            compiler_params=side,
        )(x_loc, dy_loc, idx_t, key_t, wgt, gelu_loc, lin_loc, out_loc)

        table, g0, g1, go = pl.pallas_call(
            functools.partial(expert_kernel, n_tp, n_ep),
            name="moe_expert",
            out_shape=(sds((n_tp * n_ep, cap, 128), BF16), sds((n_tp, d_model, part), BF16), sds((n_tp, d_model, part), BF16), sds((width, d_model), BF16)),
            in_specs=[vmem] * 5,
            out_specs=(hbm, vmem, vmem, vmem),
            scratch_shapes=[pltpu.VMEM((d_model, width), BF16), pltpu.VMEM((d_model, width), BF16),
                            pltpu.VMEM((cap, width), BF16), pltpu.VMEM((cap, width), BF16), pltpu.VMEM((cap, width), BF16),
                            pltpu.VMEM((d_model, width), F32), pltpu.VMEM((d_model, width), F32), pltpu.VMEM((width, d_model), F32),
                            pltpu.VMEM((n_tp, n_ep, cap, 128), BF16),
                            dma((n_tp, n_ep)), dma((n_tp, n_ep)), dma(())],
            compiler_params=side,
        )(rows, drows, w0, w1, wo.reshape(width, d_model))

        col0 = s * (d_model // n_tp)
        wg_cols = jnp.pad(lax.dynamic_slice_in_dim(wgt, col0, d_model // n_tp, axis=1), ((0, 0), (0, 64)))
        gy, gx, grad_gelu, grad_lin, grad_out, dwg_t, aux = pl.pallas_call(
            functools.partial(return_kernel, n_tp, n_ep),
            name="moe_return",
            out_shape=(sds((n_tp, tokens // 2, 128), BF16), sds((n_tp, tokens // 2, 128), BF16),
                       sds(gelu_loc.shape, BF16), sds(lin_loc.shape, BF16), sds(out_loc.shape, BF16),
                       sds((experts, d_model), F32), sds((8, 128), F32)),
            in_specs=[pl.BlockSpec(memory_space=pltpu.SMEM)] + [vmem] * 7 + [hbm] * 5,
            out_specs=(hbm, hbm, hbm, hbm, hbm, vmem, vmem),
            scratch_shapes=[pltpu.VMEM((n_tp * n_ep, cap, 128), BF16), pltpu.VMEM((slots + 8, 128), F32),
                            pltpu.VMEM((tokens, 128), F32), pltpu.VMEM((tokens, 128), F32),
                            pltpu.VMEM((tokens // 2, 128), BF16), pltpu.VMEM((tokens // 2, 128), F32), pltpu.VMEM((8, tokens // 4), F32),
                            pltpu.VMEM((tokens, d_model), BF16), dma((8,)),
                            pltpu.VMEM((n_tp, 8, tokens // 4), F32), pltpu.VMEM((tokens // 2, 128), BF16),
                            pltpu.VMEM((3 * experts, tokens), BF16), pltpu.VMEM((experts, d_model), F32), pltpu.VMEM((n_ep, experts, d_model), F32),
                            dma((3, n_tp)), dma((3, n_tp)), dma((n_tp,)), dma((n_tp,)),
                            dma((2, n_tp, 3)), dma((2, n_tp)), dma((n_ep,)), dma((n_ep,)), dma((8,))],
            compiler_params=side,
        )(pos, gate_cols, dy_cols, prob, gate, idx_t, stat, wg_cols, table, x_loc, g0, g1, go.reshape(out_loc.shape))

        pair = pl.BlockSpec((2, tokens // 2, 128), lambda j: (j, 0, 0))
        cols = pl.BlockSpec((tokens, 128), lambda j: (0, j))
        y_loc, dx_loc = pl.pallas_call(
            interleave_kernel,
            name="moe_interleave",
            grid=(n_tp // 2,),
            out_shape=(sds((tokens, d_model), BF16), sds((tokens, d_model), BF16)),
            in_specs=[pair, pair],
            out_specs=(cols, cols),
            compiler_params=pltpu.CompilerParams(dimension_semantics=("arbitrary",), vmem_limit_bytes=VMEM_LIMIT),
        )(gy, gx)
        return y_loc, dx_loc, grad_gelu, grad_lin, grad_out, dwg_t.T, aux[0, 0]

    rows_spec = P("ep", None)
    weight_in = P("ep", None, "tp")
    weight_out = P("ep", "tp", None)
    return jax.shard_map(
        device_step,
        mesh=mesh,
        in_specs=(rows_spec, P(None, None), rows_spec, rows_spec, weight_in, weight_in, weight_out, rows_spec),
        out_specs=(rows_spec, rows_spec, weight_in, weight_in, weight_out, P(None, None), P()),
        check_vma=False,
    )
```

```python
import functools

import jax
import jax.numpy as jnp
from jax import lax
from jax.experimental import pallas as pl
from jax.experimental.pallas import tpu as pltpu
from jax.sharding import PartitionSpec as P

AUX_WEIGHT = 0.01
F32 = jnp.float32
BF16 = jnp.bfloat16
VMEM_LIMIT = 64000 * 1024
GELU_C = 0.7978845608028654
GELU_A = 0.044715
ANY = pl.ANY


def dot_nn(a, b):
    return lax.dot_general(a, b, (((1,), (0,)), ((), ())), preferred_element_type=F32)


def dot_nt(a, b):
    return lax.dot_general(a, b, (((1,), (1,)), ((), ())), preferred_element_type=F32)


def dot_tn(a, b):
    return lax.dot_general(a, b, (((0,), (0,)), ((), ())), preferred_element_type=F32)


def split3(v):
    hi = v.astype(BF16)
    rest = v - hi.astype(F32)
    mid = rest.astype(BF16)
    lo = (rest - mid.astype(F32)).astype(BF16)
    return hi, mid, lo


def remote(src, dst, send_sem, recv_sem, tp, ep):
    return pltpu.make_async_remote_copy(
        src_ref=src, dst_ref=dst, send_sem=send_sem, recv_sem=recv_sem,
        device_id={"tp": tp, "ep": ep}, device_id_type=pl.DeviceIdType.MESH,
    )


def dispatch_kernel(n_tp, n_ep, cap, x_ref, dy_ref, idx_ref, key_ref, wgt_ref, w0_ref, w1_ref, wo_ref,
                    r_out, d_out, w0_out, w1_out, wo_out, prob_out, gate_out, stat_out, dyc_out, gcol_out,
                    x_buf, dy_buf, rbuf, dbuf, stat_buf, acc_r, acc_d, w_send, w_recv, row_send, row_recv, st_send, st_recv, loc_sem):
    s = lax.axis_index("tp")
    q = lax.axis_index("ep")
    tokens = x_ref.shape[0]
    experts = n_tp * n_ep
    weights = ((w0_ref, w0_out), (w1_ref, w1_out), (wo_ref, wo_out))
    copies = []
    for a, (src, dst) in enumerate(weights):
        for p in range(1, n_tp):
            peer = lax.rem(s + p, n_tp)
            copies.append(remote(src.at[peer], dst.at[s], w_send.at[a, p], w_recv.at[a, p], peer, q))
            copies[-1].start()
    x_load = pltpu.make_async_copy(x_ref, x_buf, loc_sem.at[6])
    dy_load = pltpu.make_async_copy(dy_ref, dy_buf, loc_sem.at[7])
    x_load.start()
    dy_load.start()
    local = []
    for a, (src, dst) in enumerate(weights):
        local.append(pltpu.make_async_copy(src.at[s], dst.at[s], loc_sem.at[a]))
        local[-1].start()

    hi, mid, lo = split3(wgt_ref[...])
    parts = jnp.concatenate([hi, mid, lo], axis=0)
    chunk = 1024
    e_iota = lax.broadcasted_iota(jnp.int32, (experts, chunk), 0)
    psum = jnp.zeros((experts, 1), F32)
    count = jnp.zeros((experts, 1), F32)
    x_load.wait()
    for c in range(tokens // chunk):
        cols = pl.ds(c * chunk, chunk)
        lg = dot_nt(parts, x_buf[cols, :])
        logits = lg[:experts] + (lg[experts:2 * experts] + lg[2 * experts:])
        ex = jnp.exp(logits - jnp.max(logits, axis=0, keepdims=True))
        prob = ex / jnp.sum(ex, axis=0, keepdims=True)
        prob_out[:, cols] = prob
        hot1 = e_iota == idx_ref[0:1, cols]
        hot2 = e_iota == idx_ref[1:2, cols]
        g1 = jnp.sum(jnp.where(hot1, prob, 0.0), axis=0, keepdims=True)
        g2 = jnp.sum(jnp.where(hot2, prob, 0.0), axis=0, keepdims=True)
        total = g1 + g2
        gate_out[0:1, cols] = g1 / total
        gate_out[1:2, cols] = g2 / total
        gate_out[2:3, cols] = total
        gate_out[3:8, cols] = jnp.zeros((5, chunk), F32)
        psum = psum + jnp.sum(prob, axis=1, keepdims=True)
        count = count + jnp.sum(jnp.where(hot1, 1.0, 0.0), axis=1, keepdims=True)
    lane = lax.broadcasted_iota(jnp.int32, (experts, 128), 1)
    stat_buf[...] = jnp.where(lane == 0, count, jnp.where(lane == 1, psum, 0.0))
    for p in range(1, n_ep):
        copies.append(remote(stat_buf, stat_out.at[q], st_send.at[p], st_recv.at[p], s, lax.rem(q + p, n_ep)))
        copies[-1].start()
    local.append(pltpu.make_async_copy(stat_buf, stat_out.at[q], loc_sem.at[3]))
    local[-1].start()

    def row_copies(p, r):
        return (remote(rbuf.at[p], r_out.at[q], row_send.at[0, p], row_recv.at[0, p], s, r),
                remote(dbuf.at[p], d_out.at[q], row_send.at[1, p], row_recv.at[1, p], s, r))

    def own_copies():
        return (pltpu.make_async_copy(rbuf.at[0], r_out.at[q], loc_sem.at[4]),
                pltpu.make_async_copy(dbuf.at[0], d_out.at[q], loc_sem.at[5]))

    tchunk = 512
    dy_load.wait()

    def do_dest(i, _):
        p = lax.rem(i + 1, n_ep)
        r = lax.rem(q + p, n_ep)
        base = (r * n_tp + s) * cap
        acc_r[...] = jnp.zeros_like(acc_r)
        acc_d[...] = jnp.zeros_like(acc_d)

        def do_chunk(c, gsum):
            cols = pl.ds(pl.multiple_of(c * tchunk, tchunk), tchunk)
            slot = lax.broadcasted_iota(jnp.int32, (cap, tchunk), 0)
            m1 = (key_ref[0:1, cols] - base) == slot
            m2 = (key_ref[1:2, cols] - base) == slot
            pick = jnp.where(m1 | m2, 1.0, 0.0).astype(BF16)
            acc_r[...] += dot_nn(pick, x_buf[cols, :])
            acc_d[...] += dot_nn(pick, dy_buf[cols, :])
            gsel = jnp.where(m1, gate_out[0:1, cols], 0.0) + jnp.where(m2, gate_out[1:2, cols], 0.0)
            return gsum + jnp.sum(gsel, axis=1, keepdims=True)

        gsum = lax.fori_loop(0, tokens // tchunk, do_chunk, jnp.zeros((cap, 1), F32))
        rbuf[p] = acc_r[...].astype(BF16)
        dbuf[p] = (acc_d[...] * gsum).astype(BF16)

        @pl.when(p > 0)
        def _():
            for cp in row_copies(p, r):
                cp.start()

        @pl.when(p == 0)
        def _():
            for cp in own_copies():
                cp.start()

        return 0

    lax.fori_loop(0, n_ep, do_dest, 0)

    pair = pl.ds(pl.multiple_of((s // 2) * 128, 128), 128)
    odd = lax.rem(s, 2) == 1
    for c in range(tokens // chunk):
        cols = pl.ds(c * chunk, chunk)
        dyc = dy_buf[cols, pair].astype(F32)
        dyc_out[cols, :] = jnp.where(odd, pltpu.roll(dyc, 64, 1), dyc).astype(BF16)
        gcol_out[cols, :] = gate_out[:, cols].T
    for cp in own_copies():
        cp.wait()
    for cp in local:
        cp.wait()
    for p in range(1, n_ep):
        for cp in row_copies(p, lax.rem(q + p, n_ep)):
            cp.wait()
    for cp in copies:
        cp.wait()


def expert_kernel(n_tp, n_ep, r_ref, d_ref, w0_ref, w1_ref, wo_ref, table_out, g0_out, g1_out, go_out, p0_out, p1_out, po_out,
                  w0c, w1c, h_s, da_s, db_s, acc0, acc1, acco, back, send, recv, loc, p_send, p_recv):
    s = lax.axis_index("tp")
    q = lax.axis_index("ep")
    me = s * n_ep + q
    rows, d_model = r_ref.shape[1], r_ref.shape[2]
    width = wo_ref.shape[0]
    part = width // n_tp
    for j in range(n_tp):
        w0c[:, j * part:(j + 1) * part] = w0_ref[j]
        w1c[:, j * part:(j + 1) * part] = w1_ref[j]
    acc0[...] = jnp.zeros_like(acc0)
    acc1[...] = jnp.zeros_like(acc1)
    acco[...] = jnp.zeros_like(acco)

    def row_copy(a, b):
        tp, ep = lax.rem(s + a, n_tp), lax.rem(q + b, n_ep)
        return remote(back.at[tp, ep], table_out.at[me], send.at[a, b], recv.at[a, b], tp, ep)

    own = pltpu.make_async_copy(back.at[s, q], table_out.at[me], loc)

    def shard(i, _):
        b = lax.rem(i + 1, n_ep)
        ep = lax.rem(q + b, n_ep)
        r = r_ref[ep]
        d = d_ref[ep]
        blk = 256
        for j in range(width // blk):
            sl = slice(j * blk, (j + 1) * blk)
            u = dot_nn(r, w0c[:, sl])
            v = dot_nn(r, w1c[:, sl])
            dh = dot_nt(d, wo_ref[sl, :])
            u2 = u * u
            t = jnp.tanh(GELU_C * (u + GELU_A * (u2 * u)))
            cdf = 0.5 * (1.0 + t)
            g = u * cdf
            h_s[:, sl] = (g * v).astype(BF16)
            db_s[:, sl] = (dh * g).astype(BF16)
            slope = cdf + u * (0.5 * (1.0 - t * t) * (GELU_C * (1.0 + (3.0 * GELU_A) * u2)))
            da_s[:, sl] = (dh * v * slope).astype(BF16)
        o = dot_nn(h_s[...], wo_ref[...]).astype(BF16).astype(F32)
        dr = (dot_nt(da_s[...], w0c[...]) + dot_nt(db_s[...], w1c[...])).astype(BF16).astype(F32)
        low = lax.broadcasted_iota(jnp.int32, (rows, 128), 1) < 64
        for j in range(d_model // 128):
            o_blk = o[:, j * 128:(j + 1) * 128]
            r_blk = dr[:, j * 128:(j + 1) * 128]
            back[2 * j, ep] = jnp.where(low, o_blk, pltpu.roll(r_blk, 64, 1)).astype(BF16)
            back[2 * j + 1, ep] = jnp.where(low, pltpu.roll(o_blk, 64, 1), r_blk).astype(BF16)
        for a in range(1, n_tp):
            row_copy(a, b).start()

        @pl.when(b > 0)
        def _():
            row_copy(0, b).start()

        @pl.when(b == 0)
        def _():
            own.start()

        acco[...] += dot_tn(h_s[...], d)
        acc0[...] += dot_tn(r, da_s[...])
        acc1[...] += dot_tn(r, db_s[...])
        return 0

    lax.fori_loop(0, n_ep, shard, 0)
    for j in range(n_tp):
        g0_out[j] = acc0[:, j * part:(j + 1) * part].astype(BF16)
        g1_out[j] = acc1[:, j * part:(j + 1) * part].astype(BF16)
    for j in range(n_tp):
        go_out[j] = acco[j * part:(j + 1) * part, :].astype(BF16)
    y = lax.rem(s, 2)
    crossing = []
    for a, (src, dst) in enumerate(((g0_out, p0_out), (g1_out, p1_out), (go_out, po_out))):
        for k in range(n_tp // 2):
            crossing.append(remote(src.at[2 * k + 1 - y], dst.at[k], p_send.at[a, k], p_recv.at[a, k], s + 1 - 2 * y, q))
            crossing[-1].start()
    own.wait()
    for b in range(n_ep):
        for a in range(n_tp):
            if a + b > 0:
                row_copy(a, b).wait()
    for cp in crossing:
        cp.wait()


def return_kernel(n_tp, n_ep, pos_ref, gcol_ref, dyc_ref, prob_ref, gate_ref, idx_ref, stat_ref, wgt_ref,
                  table_ref, x_ref, g0_ref, g1_ref, go_ref, p0_ref, p1_ref, po_ref,
                  gy_out, gx_out, g0_out, g1_out, go_out, dwg_out, aux_out,
                  tab_in, tab, c1, c2, y_buf, dr_buf, dg_buf, x_buf, tab_sem,
                  dg_all, dx_buf, dl_buf, dwg_buf, dwg_all,
                  stay_w, stay_o, g_send, g_recv, g_loc, dg_send, dg_recv, ag_send, ag_recv, ag_loc, wg_send, wg_recv, loc):
    s = lax.axis_index("tp")
    q = lax.axis_index("ep")
    n_z = n_tp // 2
    z = s // 2
    y = lax.rem(s, 2)
    tokens = x_ref.shape[0]
    experts = n_tp * n_ep
    total_tokens = float(tokens * n_ep)
    half = tokens // 2
    copies = []
    local = []
    grads = ((g0_ref, p0_ref, g0_out), (g1_ref, p1_ref, g1_out), (go_ref, po_ref, go_out))
    queue = [(a, h, p) for a in range(3) for p in range(1, n_z) for h in range(2)]

    def send_grads(n):
        for _ in range(min(n, len(queue))):
            a, h, p = queue.pop(0)
            own, other, dst = grads[a]
            k = lax.rem(z + p, n_z)
            src = other.at[k] if h else own.at[2 * k + y]
            source = s + 1 - 2 * y if h else s
            cp = remote(src, dst.at[source], g_send.at[a, h, p], g_recv.at[a, h, p], 2 * k + y, q)
            cp.start()
            copies.append(cp)

    stay_in, stay_out = [], []
    for a, (own, other, dst) in enumerate(grads):
        for h, (src, source) in enumerate(((own.at[s], s), (other.at[z], s + 1 - 2 * y))):
            mid = stay_o.at[h] if a == 2 else stay_w.at[a, h]
            stay_in.append(pltpu.make_async_copy(src, mid, g_loc.at[a, h]))
            stay_out.append(pltpu.make_async_copy(mid, dst.at[source], g_loc.at[a, 2 + h]))
    for cp in stay_in:
        cp.start()

    class Gather:
        def __init__(self, a, out, rows):
            self.a, self.out, self.rows = a, out, rows

        def blk(self, owner):
            return self.out.at[owner, self.rows]

        def hop(self, src, owner, way, tp):
            return remote(src, self.blk(owner), ag_send.at[self.a, owner, way], ag_recv.at[self.a, owner], tp, q)

        def up(self, src, owner):
            return self.hop(src, owner, 0, lax.rem(s + 2, n_tp))

        def down(self, src, owner):
            return self.hop(src, owner, 1, lax.rem(s + n_tp - 2, n_tp))

        def across(self, src, owner):
            return self.hop(src, owner, 2, s + 1 - 2 * y)

        def begin(self, src):
            src = src.at[self.rows]
            self.src = src
            self.own = pltpu.make_async_copy(src, self.blk(s), ag_loc.at[self.a])

            @pl.when(z < n_z - 1)
            def _():
                self.up(src, s).start()

            @pl.when(z > 0)
            def _():
                self.down(src, s).start()

            self.across(src, s).start()
            self.own.start()

        def relay(self, dist):
            @pl.when(z >= dist)
            def _():
                owner = lax.rem(s + n_tp - 2 * dist, n_tp)
                blk = self.blk(owner)
                self.up(blk, owner).wait_recv()

                @pl.when(z < n_z - 1)
                def _():
                    self.up(blk, owner).start()

                self.across(blk, owner).start()

            @pl.when(z + dist < n_z)
            def _():
                owner = lax.rem(s + 2 * dist, n_tp)
                blk = self.blk(owner)
                self.down(blk, owner).wait_recv()

                @pl.when(z > 0)
                def _():
                    self.down(blk, owner).start()

                self.across(blk, owner).start()

        def finish(self):
            @pl.when(z < n_z - 1)
            def _():
                self.up(self.src, s).wait_send()

            @pl.when(z > 0)
            def _():
                self.down(self.src, s).wait_send()

            self.across(self.src, s).wait_send()
            self.own.wait()
            for dist in range(1, n_z):
                @pl.when(z >= dist)
                def _():
                    owner = lax.rem(s + n_tp - 2 * dist, n_tp)
                    blk = self.blk(owner)

                    @pl.when(z < n_z - 1)
                    def _():
                        self.up(blk, owner).wait_send()

                    self.across(blk, owner).wait_send()

                @pl.when(z + dist < n_z)
                def _():
                    owner = lax.rem(s + 2 * dist, n_tp)
                    blk = self.blk(owner)

                    @pl.when(z > 0)
                    def _():
                        self.down(blk, owner).wait_send()

                    self.across(blk, owner).wait_send()

            for k in range(n_z):
                owner = 2 * k + 1 - y
                self.across(self.blk(owner), owner).wait_recv()

    quarter = half // 2
    gat_y = [Gather(h, gy_out, pl.ds(h * quarter, quarter)) for h in range(2)]
    gat_x = [Gather(2 + h, gx_out, pl.ds(h * quarter, quarter)) for h in range(2)]
    slots = tab_in.shape[0] * tab_in.shape[1]
    cap = tab_in.shape[1]
    groups = 8
    per = tab_in.shape[0] // groups
    loads = [pltpu.make_async_copy(table_ref.at[pl.ds(k * per, per)], tab_in.at[pl.ds(k * per, per)], tab_sem.at[k]) for k in range(groups)]
    for cp in loads:
        cp.start()
    x_load = pltpu.make_async_copy(x_ref, x_buf, loc.at[7])
    x_load.start()
    send_grads(6)

    tab[pl.ds(slots, 8), :] = jnp.zeros((8, 128), F32)
    for k in range(groups):
        loads[k].wait()

        def widen(i, _):
            tab[pl.ds(pl.multiple_of((k * per + i) * cap, cap), cap), :] = tab_in[k * per + i].astype(F32)
            return 0

        lax.fori_loop(0, per, widen, 0)

    unroll = 16

    def look(i, _):
        t0 = i * unroll
        for u in range(unroll):
            c1[pl.ds(t0 + u, 1), :] = tab[pl.ds(pos_ref[t0 + u], 1), :]
            c2[pl.ds(t0 + u, 1), :] = tab[pl.ds(pos_ref[tokens + t0 + u], 1), :]
        return 0

    blk = 512
    low = lax.broadcasted_iota(jnp.int32, (blk, 128), 1) < 64
    for part in range(2):
        for h in range(2):
            first = (h * half + part * quarter) // unroll
            lax.fori_loop(first, first + quarter // unroll, look, 0)
        for i in range(part * quarter // blk, (part + 1) * quarter // blk):
            pieces = []
            for h in range(2):
                t0 = h * half + i * blk
                a1 = c1[t0:t0 + blk, :]
                a2 = c2[t0:t0 + blk, :]
                dy = dyc_ref[t0:t0 + blk, :].astype(F32)
                pieces.append((gcol_ref[t0:t0 + blk, 0:1] * a1 + gcol_ref[t0:t0 + blk, 1:2] * a2, a1 + a2))
                prod = jnp.where(low, dy * a1, pltpu.roll(dy * a2, 64, 1)).T
                row = t0 // 1024
                col = t0 % 1024
                dg_buf[row:row + 1, col:col + blk] = jnp.sum(prod[:64], axis=0, keepdims=True)
                dg_buf[4 + row:5 + row, col:col + blk] = jnp.sum(prod[64:], axis=0, keepdims=True)
            (ya, da), (yb, db) = pieces
            y_buf[i * blk:(i + 1) * blk, :] = jnp.where(low, ya, pltpu.roll(yb, 64, 1)).astype(BF16)
            dr_buf[i * blk:(i + 1) * blk, :] = jnp.where(low, pltpu.roll(da, 64, 1), db)
        gat_y[part].begin(y_buf)

    for cin, cout in zip(stay_in, stay_out):
        cin.wait()
        cout.start()
    local.extend(stay_out)
    dg_copies = []
    for p in range(1, n_tp):
        peer = lax.rem(s + p, n_tp)
        dg_copies.append(remote(dg_buf, dg_all.at[s], dg_send.at[p], dg_recv.at[p], peer, q))
        dg_copies[-1].start()
    dg_own = pltpu.make_async_copy(dg_buf, dg_all.at[s], loc.at[0])
    dg_own.start()
    gat_y[0].relay(1)

    counts = stat_ref[0, :, 0:1]
    sums = stat_ref[0, :, 1:2]
    for e in range(1, n_ep):
        counts = counts + stat_ref[e, :, 0:1]
        sums = sums + stat_ref[e, :, 1:2]
    aux_out[0, 0] = jnp.sum(counts * sums) * (experts / (total_tokens * total_tokens))
    aux_cot = counts * (AUX_WEIGHT * experts / (total_tokens * total_tokens))
    for cp in dg_copies:
        cp.wait_recv()
    dg_own.wait()
    chunk = 1024
    e_iota = lax.broadcasted_iota(jnp.int32, (experts, chunk), 0)
    for c in range(tokens // chunk):
        cols = pl.ds(c * chunk, chunk)
        dw1 = dg_all[0, c:c + 1, :]
        dw2 = dg_all[0, 4 + c:5 + c, :]
        for o in range(1, n_tp):
            dw1 = dw1 + dg_all[o, c:c + 1, :]
            dw2 = dw2 + dg_all[o, 4 + c:5 + c, :]
        w1 = gate_ref[0:1, cols]
        w2 = gate_ref[1:2, cols]
        tot = gate_ref[2:3, cols]
        mean = dw1 * w1 + dw2 * w2
        dg1 = (dw1 - mean) / tot
        dg2 = (dw2 - mean) / tot
        prob = prob_ref[:, cols]
        dp = jnp.where(e_iota == idx_ref[0:1, cols], dg1, 0.0) + jnp.where(e_iota == idx_ref[1:2, cols], dg2, 0.0) + aux_cot
        dl = prob * (dp - jnp.sum(prob * dp, axis=0, keepdims=True))
        hi, mid, lo = split3(dl)
        dl_buf[0:experts, cols] = hi
        dl_buf[experts:2 * experts, cols] = mid
        dl_buf[2 * experts:, cols] = lo

    wcols = wgt_ref[:, pl.ds(pl.multiple_of((s // 2) * 128, 128), 128)]
    wcols = jnp.where(y == 1, pltpu.roll(wcols, 64, 1), wcols)
    wcols = jnp.where(lax.broadcasted_iota(jnp.int32, wcols.shape, 1) < 64, wcols, 0.0)
    whi, wmid, wlo = split3(wcols)
    left = lax.broadcasted_iota(jnp.int32, (half, 128), 1) < 64
    w_top = jnp.concatenate([whi, whi, whi], axis=0)
    w_mid = jnp.concatenate([wmid, wmid], axis=0)
    dl_all = dl_buf[...]
    xr = dot_tn(dl_all, w_top) + dot_tn(dl_all[:2 * experts], w_mid) + dot_tn(dl_all[:experts], wlo)
    xr = jnp.where(left, xr[:half], pltpu.roll(xr[half:], 64, 1))
    dx_buf[...] = (dr_buf[...] + xr).astype(BF16)
    gat_x[0].begin(dx_buf)
    gat_x[1].begin(dx_buf)
    gat_y[1].relay(1)
    x_load.wait()
    dw = dot_nn(dl_all, x_buf[...])
    dwg_buf[...] = dw[:experts] + (dw[experts:2 * experts] + dw[2 * experts:])
    wg_copies = []
    for p in range(1, n_ep):
        cp = remote(dwg_buf, dwg_all.at[q], wg_send.at[p], wg_recv.at[p], s, lax.rem(q + p, n_ep))
        cp.start()
        wg_copies.append(cp)
    wg_own = pltpu.make_async_copy(dwg_buf, dwg_all.at[q], loc.at[6])
    wg_own.start()
    gat_y[0].relay(2)
    gat_y[1].relay(2)
    gat_x[0].relay(1)
    gat_y[0].relay(3)
    gat_x[1].relay(1)
    gat_y[1].relay(3)
    send_grads(3)
    gat_x[0].relay(2)
    send_grads(3)
    gat_x[1].relay(2)
    send_grads(3)
    gat_x[0].relay(3)
    gat_x[1].relay(3)
    send_grads(3)
    wg_own.wait()
    for cp in wg_copies:
        cp.wait()
    tot = dwg_all[0]
    for e in range(1, n_ep):
        tot = tot + dwg_all[e]
    dwg_out[...] = tot
    for gat in gat_y + gat_x:
        gat.finish()
    for cp in dg_copies:
        cp.wait_send()
    for cp in local:
        cp.wait()
    for cp in copies:
        cp.wait()


def interleave_kernel(gy_ref, gx_ref, g0_ref, g1_ref, go_ref, y_out, dx_out, g0_out, g1_out, go_out):
    half = gy_ref.shape[1]
    low = lax.broadcasted_iota(jnp.int32, (half, 128), 1) < 64
    for src, dst in ((gy_ref, y_out), (gx_ref, dx_out)):
        a = src[0].astype(F32)
        b = src[1].astype(F32)
        dst[0:half, :] = jnp.where(low, a, pltpu.roll(b, 64, 1)).astype(BF16)
        dst[half:2 * half, :] = jnp.where(low, pltpu.roll(a, 64, 1), b).astype(BF16)
    g0_out[...] = g0_ref[...]
    g1_out[...] = g1_ref[...]
    go_out[...] = go_ref[...]


def solution(mesh):
    n_ep = mesh.shape["ep"]
    n_tp = mesh.shape["tp"]
    vmem = pl.BlockSpec(memory_space=pltpu.VMEM)
    hbm = pl.BlockSpec(memory_space=ANY)
    dma = pltpu.SemaphoreType.DMA
    sds = jax.ShapeDtypeStruct

    def device_step(x_loc, w_router, idx_loc, slot_loc, gelu_loc, lin_loc, out_loc, dy_loc):
        tokens, d_model = x_loc.shape
        exp_local = gelu_loc.shape[0]
        part = gelu_loc.shape[2]
        width = part * n_tp
        experts = exp_local * n_ep
        cap = 4 * tokens // experts
        slots = experts * cap
        s = lax.axis_index("tp")
        idx_t = idx_loc.T
        slot_t = slot_loc.T
        kept = slot_t < cap
        key_t = jnp.where(kept, idx_t * cap + slot_t, -1)
        pos = jnp.where(kept, ((idx_t % n_tp) * n_ep + idx_t // n_tp) * cap + slot_t, slots).reshape(-1)
        wgt = w_router.T
        side = pltpu.CompilerParams(has_side_effects=True, vmem_limit_bytes=VMEM_LIMIT)

        rows, drows, w0, w1, wo, prob, gate, stat, dy_cols, gate_cols = pl.pallas_call(
            functools.partial(dispatch_kernel, n_tp, n_ep, cap),
            name="moe_dispatch",
            out_shape=(sds((n_ep, cap, d_model), BF16), sds((n_ep, cap, d_model), BF16),
                       sds(gelu_loc.shape, BF16), sds(lin_loc.shape, BF16), sds(out_loc.shape, BF16),
                       sds((experts, tokens), F32), sds((8, tokens), F32), sds((n_ep, experts, 128), F32),
                       sds((tokens, 128), BF16), sds((tokens, 8), F32)),
            in_specs=[hbm] * 2 + [vmem] * 3 + [hbm] * 3,
            out_specs=(hbm, hbm, hbm, hbm, hbm, vmem, vmem, vmem, vmem, vmem),
            scratch_shapes=[pltpu.VMEM((tokens, d_model), BF16), pltpu.VMEM((tokens, d_model), BF16),
                            pltpu.VMEM((n_ep, cap, d_model), BF16), pltpu.VMEM((n_ep, cap, d_model), BF16),
                            pltpu.VMEM((experts, 128), F32), pltpu.VMEM((cap, d_model), F32), pltpu.VMEM((cap, d_model), F32),
                            dma((3, n_tp)), dma((3, n_tp)), dma((2, n_ep)), dma((2, n_ep)), dma((n_ep,)), dma((n_ep,)), dma((8,))],
            compiler_params=side,
        )(x_loc, dy_loc, idx_t, key_t, wgt, gelu_loc, lin_loc, out_loc)

        half_shape = lambda ref: sds((n_tp // 2,) + ref.shape[1:], BF16)
        table, g0, g1, go, p0, p1, po = pl.pallas_call(
            functools.partial(expert_kernel, n_tp, n_ep),
            name="moe_expert",
            out_shape=(sds((n_tp * n_ep, cap, 128), BF16), sds(gelu_loc.shape, BF16), sds(lin_loc.shape, BF16), sds(out_loc.shape, BF16),
                       half_shape(gelu_loc), half_shape(lin_loc), half_shape(out_loc)),
            in_specs=[vmem] * 5,
            out_specs=(hbm, vmem, vmem, vmem, hbm, hbm, hbm),
            scratch_shapes=[pltpu.VMEM((d_model, width), BF16), pltpu.VMEM((d_model, width), BF16),
                            pltpu.VMEM((cap, width), BF16), pltpu.VMEM((cap, width), BF16), pltpu.VMEM((cap, width), BF16),
                            pltpu.VMEM((d_model, width), F32), pltpu.VMEM((d_model, width), F32), pltpu.VMEM((width, d_model), F32),
                            pltpu.VMEM((n_tp, n_ep, cap, 128), BF16),
                            dma((n_tp, n_ep)), dma((n_tp, n_ep)), dma(()), dma((3, n_tp // 2)), dma((3, n_tp // 2))],
            compiler_params=side,
        )(rows, drows, w0, w1, wo.reshape(width, d_model))

        gy, gx, grad_gelu, grad_lin, grad_out, dwg_t, aux = pl.pallas_call(
            functools.partial(return_kernel, n_tp, n_ep),
            name="moe_return",
            out_shape=(sds((n_tp, tokens // 2, 128), BF16), sds((n_tp, tokens // 2, 128), BF16),
                       sds(gelu_loc.shape, BF16), sds(lin_loc.shape, BF16), sds(out_loc.shape, BF16),
                       sds((experts, d_model), F32), sds((1, 1), F32)),
            in_specs=[pl.BlockSpec(memory_space=pltpu.SMEM)] + [vmem] * 7 + [hbm] * 8,
            out_specs=(hbm, hbm, hbm, hbm, hbm, vmem, pl.BlockSpec(memory_space=pltpu.SMEM)),
            scratch_shapes=[pltpu.VMEM((n_tp * n_ep, cap, 128), BF16), pltpu.VMEM((slots + 8, 128), F32),
                            pltpu.VMEM((tokens, 128), F32), pltpu.VMEM((tokens, 128), F32),
                            pltpu.VMEM((tokens // 2, 128), BF16), pltpu.VMEM((tokens // 2, 128), F32), pltpu.VMEM((8, tokens // 4), F32),
                            pltpu.VMEM((tokens, d_model), BF16), dma((8,)),
                            pltpu.VMEM((n_tp, 8, tokens // 4), F32), pltpu.VMEM((tokens // 2, 128), BF16),
                            pltpu.VMEM((3 * experts, tokens), BF16), pltpu.VMEM((experts, d_model), F32), pltpu.VMEM((n_ep, experts, d_model), F32),
                            pltpu.VMEM((2, 2, d_model, part), BF16), pltpu.VMEM((2, part, d_model), BF16),
                            dma((3, 2, n_tp // 2)), dma((3, 2, n_tp // 2)), dma((3, 4)), dma((n_tp,)), dma((n_tp,)),
                            dma((4, n_tp, 3)), dma((4, n_tp)), dma((4,)), dma((n_ep,)), dma((n_ep,)), dma((8,))],
            compiler_params=side,
        )(pos, gate_cols, dy_cols, prob, gate, idx_t, stat, wgt, table, x_loc, g0, g1, go, p0, p1, po)

        pair = pl.BlockSpec((2, tokens // 2, 128), lambda j: (j, 0, 0))
        cols = pl.BlockSpec((tokens, 128), lambda j: (0, j))
        block = lambda ref: pl.BlockSpec((2,) + ref.shape[1:], lambda j: (j, 0, 0))
        y_loc, dx_loc, grad_gelu, grad_lin, grad_out = pl.pallas_call(
            interleave_kernel,
            name="moe_interleave",
            grid=(n_tp // 2,),
            out_shape=(sds((tokens, d_model), BF16), sds((tokens, d_model), BF16), sds(gelu_loc.shape, BF16), sds(lin_loc.shape, BF16), sds(out_loc.shape, BF16)),
            in_specs=[pair, pair, block(gelu_loc), block(lin_loc), block(out_loc)],
            out_specs=(cols, cols, block(gelu_loc), block(lin_loc), block(out_loc)),
            compiler_params=pltpu.CompilerParams(dimension_semantics=("arbitrary",), vmem_limit_bytes=VMEM_LIMIT),
        )(gy, gx, grad_gelu, grad_lin, grad_out)
        return y_loc, dx_loc, grad_gelu, grad_lin, grad_out, dwg_t.T, aux.reshape(())

    rows_spec = P("ep", None)
    weight_in = P("ep", None, "tp")
    weight_out = P("ep", "tp", None)
    return jax.shard_map(
        device_step,
        mesh=mesh,
        in_specs=(rows_spec, P(None, None), rows_spec, rows_spec, weight_in, weight_in, weight_out, rows_spec),
        out_specs=(rows_spec, rows_spec, weight_in, weight_in, weight_out, P(None, None), P()),
        check_vma=False,
    )
```

```python
import functools

import jax
import jax.numpy as jnp
from jax import lax
from jax.experimental import pallas as pl
from jax.experimental.pallas import tpu as pltpu
from jax.sharding import PartitionSpec as P

AUX_WEIGHT = 0.01
F32 = jnp.float32
BF16 = jnp.bfloat16
VMEM_LIMIT = 64000 * 1024
GELU_C = 0.7978845608028654
GELU_A = 0.044715
ANY = pl.ANY


def dot_nn(a, b):
    return lax.dot_general(a, b, (((1,), (0,)), ((), ())), preferred_element_type=F32)


def dot_nt(a, b):
    return lax.dot_general(a, b, (((1,), (1,)), ((), ())), preferred_element_type=F32)


def dot_tn(a, b):
    return lax.dot_general(a, b, (((0,), (0,)), ((), ())), preferred_element_type=F32)


def split3(v):
    hi = v.astype(BF16)
    rest = v - hi.astype(F32)
    mid = rest.astype(BF16)
    lo = (rest - mid.astype(F32)).astype(BF16)
    return hi, mid, lo


def remote(src, dst, send_sem, recv_sem, tp, ep):
    return pltpu.make_async_remote_copy(
        src_ref=src, dst_ref=dst, send_sem=send_sem, recv_sem=recv_sem,
        device_id={"tp": tp, "ep": ep}, device_id_type=pl.DeviceIdType.MESH,
    )


def dispatch_kernel(n_tp, n_ep, cap, x_ref, dy_ref, idx_ref, key_ref, wgt_ref, w0_ref, w1_ref, wo_ref,
                    r_out, d_out, w0_out, w1_out, wo_out, prob_out, gate_out, stat_out, dyc_out, gcol_out,
                    x_buf, dy_buf, rbuf, dbuf, stat_buf, acc_r, acc_d, w_send, w_recv, row_send, row_recv, st_send, st_recv, loc_sem):
    s = lax.axis_index("tp")
    q = lax.axis_index("ep")
    tokens = x_ref.shape[0]
    experts = n_tp * n_ep
    weights = ((w0_ref, w0_out), (w1_ref, w1_out), (wo_ref, wo_out))
    copies = []
    for a, (src, dst) in enumerate(weights):
        for p in range(1, n_tp):
            peer = lax.rem(s + p, n_tp)
            copies.append(remote(src.at[peer], dst.at[s], w_send.at[a, p], w_recv.at[a, p], peer, q))
            copies[-1].start()
    x_load = pltpu.make_async_copy(x_ref, x_buf, loc_sem.at[6])
    dy_load = pltpu.make_async_copy(dy_ref, dy_buf, loc_sem.at[7])
    x_load.start()
    dy_load.start()
    local = []
    for a, (src, dst) in enumerate(weights):
        local.append(pltpu.make_async_copy(src.at[s], dst.at[s], loc_sem.at[a]))
        local[-1].start()

    hi, mid, lo = split3(wgt_ref[...])
    parts = jnp.concatenate([hi, mid, lo], axis=0)
    chunk = 1024
    e_iota = lax.broadcasted_iota(jnp.int32, (experts, chunk), 0)
    psum = jnp.zeros((experts, 1), F32)
    count = jnp.zeros((experts, 1), F32)
    x_load.wait()
    for c in range(tokens // chunk):
        cols = pl.ds(c * chunk, chunk)
        lg = dot_nt(parts, x_buf[cols, :])
        logits = lg[:experts] + (lg[experts:2 * experts] + lg[2 * experts:])
        ex = jnp.exp(logits - jnp.max(logits, axis=0, keepdims=True))
        prob = ex / jnp.sum(ex, axis=0, keepdims=True)
        prob_out[:, cols] = prob
        hot1 = e_iota == idx_ref[0:1, cols]
        hot2 = e_iota == idx_ref[1:2, cols]
        g1 = jnp.sum(jnp.where(hot1, prob, 0.0), axis=0, keepdims=True)
        g2 = jnp.sum(jnp.where(hot2, prob, 0.0), axis=0, keepdims=True)
        total = g1 + g2
        gate_out[0:1, cols] = g1 / total
        gate_out[1:2, cols] = g2 / total
        gate_out[2:3, cols] = total
        gate_out[3:8, cols] = jnp.zeros((5, chunk), F32)
        psum = psum + jnp.sum(prob, axis=1, keepdims=True)
        count = count + jnp.sum(jnp.where(hot1, 1.0, 0.0), axis=1, keepdims=True)
    lane = lax.broadcasted_iota(jnp.int32, (experts, 128), 1)
    stat_buf[...] = jnp.where(lane == 0, count, jnp.where(lane == 1, psum, 0.0))
    for p in range(1, n_ep):
        copies.append(remote(stat_buf, stat_out.at[q], st_send.at[p], st_recv.at[p], s, lax.rem(q + p, n_ep)))
        copies[-1].start()
    local.append(pltpu.make_async_copy(stat_buf, stat_out.at[q], loc_sem.at[3]))
    local[-1].start()

    def row_copies(p, r):
        return (remote(rbuf.at[p], r_out.at[q], row_send.at[0, p], row_recv.at[0, p], s, r),
                remote(dbuf.at[p], d_out.at[q], row_send.at[1, p], row_recv.at[1, p], s, r))

    def own_copies():
        return (pltpu.make_async_copy(rbuf.at[0], r_out.at[q], loc_sem.at[4]),
                pltpu.make_async_copy(dbuf.at[0], d_out.at[q], loc_sem.at[5]))

    tchunk = 512
    dy_load.wait()

    def do_dest(i, _):
        p = lax.rem(i + 1, n_ep)
        r = lax.rem(q + p, n_ep)
        base = (r * n_tp + s) * cap
        acc_r[...] = jnp.zeros_like(acc_r)
        acc_d[...] = jnp.zeros_like(acc_d)

        def do_chunk(c, gsum):
            cols = pl.ds(pl.multiple_of(c * tchunk, tchunk), tchunk)
            slot = lax.broadcasted_iota(jnp.int32, (cap, tchunk), 0)
            m1 = (key_ref[0:1, cols] - base) == slot
            m2 = (key_ref[1:2, cols] - base) == slot
            pick = jnp.where(m1 | m2, 1.0, 0.0).astype(BF16)
            acc_r[...] += dot_nn(pick, x_buf[cols, :])
            acc_d[...] += dot_nn(pick, dy_buf[cols, :])
            gsel = jnp.where(m1, gate_out[0:1, cols], 0.0) + jnp.where(m2, gate_out[1:2, cols], 0.0)
            return gsum + jnp.sum(gsel, axis=1, keepdims=True)

        gsum = lax.fori_loop(0, tokens // tchunk, do_chunk, jnp.zeros((cap, 1), F32))
        rbuf[p] = acc_r[...].astype(BF16)
        dbuf[p] = (acc_d[...] * gsum).astype(BF16)

        @pl.when(p > 0)
        def _():
            for cp in row_copies(p, r):
                cp.start()

        @pl.when(p == 0)
        def _():
            for cp in own_copies():
                cp.start()

        return 0

    lax.fori_loop(0, n_ep, do_dest, 0)

    pair = pl.ds(pl.multiple_of((s // 2) * 128, 128), 128)
    odd = lax.rem(s, 2) == 1
    for c in range(tokens // chunk):
        cols = pl.ds(c * chunk, chunk)
        dyc = dy_buf[cols, pair].astype(F32)
        dyc_out[cols, :] = jnp.where(odd, pltpu.roll(dyc, 64, 1), dyc).astype(BF16)
        gcol_out[cols, :] = gate_out[:, cols].T
    for cp in own_copies():
        cp.wait()
    for cp in local:
        cp.wait()
    for p in range(1, n_ep):
        for cp in row_copies(p, lax.rem(q + p, n_ep)):
            cp.wait()
    for cp in copies:
        cp.wait()


def expert_kernel(n_tp, n_ep, r_ref, d_ref, w0_ref, w1_ref, wo_ref, table_out, g0_out, g1_out, go_out, p0_out, p1_out, po_out, n0_out, n1_out, no_out,
                  w0c, w1c, h_s, da_s, db_s, acc0, acc1, acco, back, send, recv, loc, p_send, p_recv, n_send, n_recv):
    s = lax.axis_index("tp")
    q = lax.axis_index("ep")
    me = s * n_ep + q
    rows, d_model = r_ref.shape[1], r_ref.shape[2]
    width = wo_ref.shape[0]
    part = width // n_tp
    for j in range(n_tp):
        w0c[:, j * part:(j + 1) * part] = w0_ref[j]
        w1c[:, j * part:(j + 1) * part] = w1_ref[j]
    acc0[...] = jnp.zeros_like(acc0)
    acc1[...] = jnp.zeros_like(acc1)
    acco[...] = jnp.zeros_like(acco)

    step_rows = rows // 2

    def row_copy(a, b, h):
        tp, ep = lax.rem(s + a, n_tp), lax.rem(q + b, n_ep)
        sl = pl.ds(h * step_rows, step_rows)
        return remote(back.at[tp, ep, sl], table_out.at[me, sl], send.at[h, a, b], recv.at[h, a, b], tp, ep)

    def own(h):
        sl = pl.ds(h * step_rows, step_rows)
        return pltpu.make_async_copy(back.at[s, q, sl], table_out.at[me, sl], loc.at[h])

    def half_shard(i, _):
        h = lax.rem(i, 2)
        b = lax.rem(i // 2 + 1, n_ep)
        ep = lax.rem(q + b, n_ep)
        here = pl.ds(pl.multiple_of(h * step_rows, step_rows), step_rows)
        r = r_ref[ep, here, :]
        d = d_ref[ep, here, :]
        blk = 256
        for j in range(width // blk):
            sl = slice(j * blk, (j + 1) * blk)
            u = dot_nn(r, w0c[:, sl])
            v = dot_nn(r, w1c[:, sl])
            dh = dot_nt(d, wo_ref[sl, :])
            u2 = u * u
            t = jnp.tanh(GELU_C * (u + GELU_A * (u2 * u)))
            cdf = 0.5 * (1.0 + t)
            g = u * cdf
            h_s[:, sl] = (g * v).astype(BF16)
            db_s[:, sl] = (dh * g).astype(BF16)
            slope = cdf + u * (0.5 * (1.0 - t * t) * (GELU_C * (1.0 + (3.0 * GELU_A) * u2)))
            da_s[:, sl] = (dh * v * slope).astype(BF16)
        o = dot_nn(h_s[...], wo_ref[...]).astype(BF16).astype(F32)
        dr = (dot_nt(da_s[...], w0c[...]) + dot_nt(db_s[...], w1c[...])).astype(BF16).astype(F32)
        low = lax.broadcasted_iota(jnp.int32, (step_rows, 128), 1) < 64
        for j in range(d_model // 128):
            o_blk = o[:, j * 128:(j + 1) * 128]
            r_blk = dr[:, j * 128:(j + 1) * 128]
            back[2 * j, ep, here, :] = jnp.where(low, o_blk, pltpu.roll(r_blk, 64, 1)).astype(BF16)
            back[2 * j + 1, ep, here, :] = jnp.where(low, pltpu.roll(o_blk, 64, 1), r_blk).astype(BF16)
        for a in range(1, n_tp):
            row_copy(a, b, h).start()

        @pl.when(b > 0)
        def _():
            row_copy(0, b, h).start()

        @pl.when(b == 0)
        def _():
            own(h).start()

        acco[...] += dot_tn(h_s[...], d)
        acc0[...] += dot_tn(r, da_s[...])
        acc1[...] += dot_tn(r, db_s[...])
        return 0

    lax.fori_loop(0, 2 * n_ep, half_shard, 0)
    for j in range(n_tp):
        g0_out[j] = acc0[:, j * part:(j + 1) * part].astype(BF16)
        g1_out[j] = acc1[:, j * part:(j + 1) * part].astype(BF16)
    for j in range(n_tp):
        go_out[j] = acco[j * part:(j + 1) * part, :].astype(BF16)
    y = lax.rem(s, 2)
    crossing = []
    for a, (src, dst) in enumerate(((g0_out, p0_out), (g1_out, p1_out), (go_out, po_out))):
        for k in range(n_tp // 2):
            crossing.append(remote(src.at[2 * k + 1 - y], dst.at[k], p_send.at[a, k], p_recv.at[a, k], s + 1 - 2 * y, q))
            crossing[-1].start()
    z = s // 2
    near = z + 1 - 2 * lax.rem(z, 2)
    for a, (src, dst) in enumerate(((g0_out, n0_out), (g1_out, n1_out), (go_out, no_out))):
        peer = 2 * near + y
        crossing.append(remote(src.at[peer], dst, n_send.at[a], n_recv.at[a], peer, q))
        crossing[-1].start()
    for h in range(2):
        own(h).wait()
        for b in range(n_ep):
            for a in range(n_tp):
                if a + b > 0:
                    row_copy(a, b, h).wait()
    for cp in crossing:
        cp.wait()


def return_kernel(n_tp, n_ep, pos_ref, gcol_ref, dyc_ref, prob_ref, gate_ref, idx_ref, stat_ref, wgt_ref,
                  table_ref, x_ref, g0_ref, g1_ref, go_ref, p0_ref, p1_ref, po_ref, n0_ref, n1_ref, no_ref,
                  gy_out, gx_out, g0_out, g1_out, go_out, dwg_out, aux_out,
                  tab_in, tab, c1, c2, y_buf, dr_buf, dg_buf, x_buf, tab_sem,
                  dg_all, dx_buf, dl_buf, dwg_buf, dwg_all,
                  stay_w, stay_o, g_send, g_recv, g_loc, dg_send, dg_recv, ag_send, ag_recv, ag_loc, wg_send, wg_recv, loc):
    s = lax.axis_index("tp")
    q = lax.axis_index("ep")
    n_z = n_tp // 2
    z = s // 2
    y = lax.rem(s, 2)
    tokens = x_ref.shape[0]
    experts = n_tp * n_ep
    total_tokens = float(tokens * n_ep)
    half = tokens // 2
    copies = []
    local = []
    grads = ((g0_ref, p0_ref, n0_ref, g0_out), (g1_ref, p1_ref, n1_ref, g1_out), (go_ref, po_ref, no_ref, go_out))
    queue = [(a, h, p) for a in range(3) for h, p in ((1, 1), (0, 1), (1, 2), (0, 2), (1, 3))]
    near = z + 1 - 2 * lax.rem(z, 2)

    def send_grads(n):
        for _ in range(min(n, len(queue))):
            a, h, p = queue.pop(0)
            own, other, _, dst = grads[a]
            k = lax.rem(z + p, n_z)
            if h == 0 and p == 1:
                k = lax.rem(near + 2, n_z)
            src = other.at[k] if h else own.at[2 * k + y]
            source = s + 1 - 2 * y if h else s
            cp = remote(src, dst.at[source], g_send.at[a, h, p], g_recv.at[a, h, p], 2 * k + y, q)
            cp.start()
            copies.append(cp)

    stay_in, stay_out = [], []
    for a, (own, other, close, dst) in enumerate(grads):
        for h, (src, source) in enumerate(((own.at[s], s), (other.at[z], s + 1 - 2 * y), (close, 2 * near + y))):
            mid = stay_o.at[h] if a == 2 else stay_w.at[a, h]
            stay_in.append(pltpu.make_async_copy(src, mid, g_loc.at[a, h]))
            stay_out.append(pltpu.make_async_copy(mid, dst.at[source], g_loc.at[a, 3 + h]))
    for cp in stay_in:
        cp.start()

    class Gather:
        def __init__(self, a, out, rows):
            self.a, self.out, self.rows = a, out, rows

        def blk(self, owner):
            return self.out.at[owner, self.rows]

        def hop(self, src, owner, way, tp):
            return remote(src, self.blk(owner), ag_send.at[self.a, owner, way], ag_recv.at[self.a, owner], tp, q)

        def up(self, src, owner):
            return self.hop(src, owner, 0, lax.rem(s + 2, n_tp))

        def down(self, src, owner):
            return self.hop(src, owner, 1, lax.rem(s + n_tp - 2, n_tp))

        def across(self, src, owner):
            return self.hop(src, owner, 2, s + 1 - 2 * y)

        def begin(self, src):
            src = src.at[self.rows]
            self.src = src
            self.own = pltpu.make_async_copy(src, self.blk(s), ag_loc.at[self.a])

            @pl.when(z < n_z - 1)
            def _():
                self.up(src, s).start()

            @pl.when(z > 0)
            def _():
                self.down(src, s).start()

            self.across(src, s).start()
            self.own.start()

        def relay(self, dist):
            @pl.when(z >= dist)
            def _():
                owner = lax.rem(s + n_tp - 2 * dist, n_tp)
                blk = self.blk(owner)
                self.up(blk, owner).wait_recv()

                @pl.when(z < n_z - 1)
                def _():
                    self.up(blk, owner).start()

                self.across(blk, owner).start()

            @pl.when(z + dist < n_z)
            def _():
                owner = lax.rem(s + 2 * dist, n_tp)
                blk = self.blk(owner)
                self.down(blk, owner).wait_recv()

                @pl.when(z > 0)
                def _():
                    self.down(blk, owner).start()

                self.across(blk, owner).start()

        def finish(self):
            @pl.when(z < n_z - 1)
            def _():
                self.up(self.src, s).wait_send()

            @pl.when(z > 0)
            def _():
                self.down(self.src, s).wait_send()

            self.across(self.src, s).wait_send()
            self.own.wait()
            for dist in range(1, n_z):
                @pl.when(z >= dist)
                def _():
                    owner = lax.rem(s + n_tp - 2 * dist, n_tp)
                    blk = self.blk(owner)

                    @pl.when(z < n_z - 1)
                    def _():
                        self.up(blk, owner).wait_send()

                    self.across(blk, owner).wait_send()

                @pl.when(z + dist < n_z)
                def _():
                    owner = lax.rem(s + 2 * dist, n_tp)
                    blk = self.blk(owner)

                    @pl.when(z > 0)
                    def _():
                        self.down(blk, owner).wait_send()

                    self.across(blk, owner).wait_send()

            for k in range(n_z):
                owner = 2 * k + 1 - y
                self.across(self.blk(owner), owner).wait_recv()

    quarter = half // 2
    gat_y = [Gather(h, gy_out, pl.ds(h * quarter, quarter)) for h in range(2)]
    gat_x = [Gather(2 + h, gx_out, pl.ds(h * quarter, quarter)) for h in range(2)]
    slots = tab_in.shape[0] * tab_in.shape[1]
    cap = tab_in.shape[1]
    groups = 8
    per = tab_in.shape[0] // groups
    loads = [pltpu.make_async_copy(table_ref.at[pl.ds(k * per, per)], tab_in.at[pl.ds(k * per, per)], tab_sem.at[k]) for k in range(groups)]
    for cp in loads:
        cp.start()
    x_load = pltpu.make_async_copy(x_ref, x_buf, loc.at[7])
    x_load.start()
    send_grads(5)

    tab[pl.ds(slots, 8), :] = jnp.zeros((8, 128), F32)
    for k in range(groups):
        loads[k].wait()

        def widen(i, _):
            tab[pl.ds(pl.multiple_of((k * per + i) * cap, cap), cap), :] = tab_in[k * per + i].astype(F32)
            return 0

        lax.fori_loop(0, per, widen, 0)

    unroll = 16

    def look(i, _):
        t0 = i * unroll
        for u in range(unroll):
            c1[pl.ds(t0 + u, 1), :] = tab[pl.ds(pos_ref[t0 + u], 1), :]
            c2[pl.ds(t0 + u, 1), :] = tab[pl.ds(pos_ref[tokens + t0 + u], 1), :]
        return 0

    blk = 512
    low = lax.broadcasted_iota(jnp.int32, (blk, 128), 1) < 64
    for part in range(2):
        for h in range(2):
            first = (h * half + part * quarter) // unroll
            lax.fori_loop(first, first + quarter // unroll, look, 0)
        for i in range(part * quarter // blk, (part + 1) * quarter // blk):
            pieces = []
            for h in range(2):
                t0 = h * half + i * blk
                a1 = c1[t0:t0 + blk, :]
                a2 = c2[t0:t0 + blk, :]
                dy = dyc_ref[t0:t0 + blk, :].astype(F32)
                pieces.append((gcol_ref[t0:t0 + blk, 0:1] * a1 + gcol_ref[t0:t0 + blk, 1:2] * a2, a1 + a2))
                prod = jnp.where(low, dy * a1, pltpu.roll(dy * a2, 64, 1)).T
                row = t0 // 1024
                col = t0 % 1024
                dg_buf[row:row + 1, col:col + blk] = jnp.sum(prod[:64], axis=0, keepdims=True)
                dg_buf[4 + row:5 + row, col:col + blk] = jnp.sum(prod[64:], axis=0, keepdims=True)
            (ya, da), (yb, db) = pieces
            y_buf[i * blk:(i + 1) * blk, :] = jnp.where(low, ya, pltpu.roll(yb, 64, 1)).astype(BF16)
            dr_buf[i * blk:(i + 1) * blk, :] = jnp.where(low, pltpu.roll(da, 64, 1), db)
        gat_y[part].begin(y_buf)

    for cin, cout in zip(stay_in, stay_out):
        cin.wait()
        cout.start()
    local.extend(stay_out)
    dg_copies = []
    for p in range(1, n_tp):
        peer = lax.rem(s + p, n_tp)
        dg_copies.append(remote(dg_buf, dg_all.at[s], dg_send.at[p], dg_recv.at[p], peer, q))
        dg_copies[-1].start()
    dg_own = pltpu.make_async_copy(dg_buf, dg_all.at[s], loc.at[0])
    dg_own.start()
    gat_y[0].relay(1)

    counts = stat_ref[0, :, 0:1]
    sums = stat_ref[0, :, 1:2]
    for e in range(1, n_ep):
        counts = counts + stat_ref[e, :, 0:1]
        sums = sums + stat_ref[e, :, 1:2]
    aux_out[0, 0] = jnp.sum(counts * sums) * (experts / (total_tokens * total_tokens))
    aux_cot = counts * (AUX_WEIGHT * experts / (total_tokens * total_tokens))
    for cp in dg_copies:
        cp.wait_recv()
    dg_own.wait()
    chunk = 1024
    e_iota = lax.broadcasted_iota(jnp.int32, (experts, chunk), 0)
    for c in range(tokens // chunk):
        cols = pl.ds(c * chunk, chunk)
        dw1 = dg_all[0, c:c + 1, :]
        dw2 = dg_all[0, 4 + c:5 + c, :]
        for o in range(1, n_tp):
            dw1 = dw1 + dg_all[o, c:c + 1, :]
            dw2 = dw2 + dg_all[o, 4 + c:5 + c, :]
        w1 = gate_ref[0:1, cols]
        w2 = gate_ref[1:2, cols]
        tot = gate_ref[2:3, cols]
        mean = dw1 * w1 + dw2 * w2
        dg1 = (dw1 - mean) / tot
        dg2 = (dw2 - mean) / tot
        prob = prob_ref[:, cols]
        dp = jnp.where(e_iota == idx_ref[0:1, cols], dg1, 0.0) + jnp.where(e_iota == idx_ref[1:2, cols], dg2, 0.0) + aux_cot
        dl = prob * (dp - jnp.sum(prob * dp, axis=0, keepdims=True))
        hi, mid, lo = split3(dl)
        dl_buf[0:experts, cols] = hi
        dl_buf[experts:2 * experts, cols] = mid
        dl_buf[2 * experts:, cols] = lo

    wcols = wgt_ref[:, pl.ds(pl.multiple_of((s // 2) * 128, 128), 128)]
    wcols = jnp.where(y == 1, pltpu.roll(wcols, 64, 1), wcols)
    wcols = jnp.where(lax.broadcasted_iota(jnp.int32, wcols.shape, 1) < 64, wcols, 0.0)
    whi, wmid, wlo = split3(wcols)
    left = lax.broadcasted_iota(jnp.int32, (half, 128), 1) < 64
    w_top = jnp.concatenate([whi, whi, whi], axis=0)
    w_mid = jnp.concatenate([wmid, wmid], axis=0)
    dl_all = dl_buf[...]
    xr = dot_tn(dl_all, w_top) + dot_tn(dl_all[:2 * experts], w_mid) + dot_tn(dl_all[:experts], wlo)
    xr = jnp.where(left, xr[:half], pltpu.roll(xr[half:], 64, 1))
    dx_buf[...] = (dr_buf[...] + xr).astype(BF16)
    gat_x[0].begin(dx_buf)
    gat_x[1].begin(dx_buf)
    gat_y[1].relay(1)
    x_load.wait()
    dw = dot_nn(dl_all, x_buf[...])
    dwg_buf[...] = dw[:experts] + (dw[experts:2 * experts] + dw[2 * experts:])
    wg_copies = []
    for p in range(1, n_ep):
        cp = remote(dwg_buf, dwg_all.at[q], wg_send.at[p], wg_recv.at[p], s, lax.rem(q + p, n_ep))
        cp.start()
        wg_copies.append(cp)
    wg_own = pltpu.make_async_copy(dwg_buf, dwg_all.at[q], loc.at[6])
    wg_own.start()
    gat_y[0].relay(2)
    gat_y[1].relay(2)
    gat_x[0].relay(1)
    gat_y[0].relay(3)
    gat_x[1].relay(1)
    gat_y[1].relay(3)
    send_grads(3)
    gat_x[0].relay(2)
    send_grads(2)
    gat_x[1].relay(2)
    send_grads(2)
    gat_x[0].relay(3)
    gat_x[1].relay(3)
    send_grads(3)
    wg_own.wait()
    for cp in wg_copies:
        cp.wait()
    tot = dwg_all[0]
    for e in range(1, n_ep):
        tot = tot + dwg_all[e]
    dwg_out[...] = tot
    for gat in gat_y + gat_x:
        gat.finish()
    for cp in dg_copies:
        cp.wait_send()
    for cp in local:
        cp.wait()
    for cp in copies:
        cp.wait()


def interleave_kernel(gy_ref, gx_ref, g0_ref, g1_ref, go_ref, y_out, dx_out, g0_out, g1_out, go_out):
    half = gy_ref.shape[1]
    low = lax.broadcasted_iota(jnp.int32, (half, 128), 1) < 64
    for src, dst in ((gy_ref, y_out), (gx_ref, dx_out)):
        a = src[0].astype(F32)
        b = src[1].astype(F32)
        dst[0:half, :] = jnp.where(low, a, pltpu.roll(b, 64, 1)).astype(BF16)
        dst[half:2 * half, :] = jnp.where(low, pltpu.roll(a, 64, 1), b).astype(BF16)
    g0_out[...] = g0_ref[...]
    g1_out[...] = g1_ref[...]
    go_out[...] = go_ref[...]


def solution(mesh):
    n_ep = mesh.shape["ep"]
    n_tp = mesh.shape["tp"]
    vmem = pl.BlockSpec(memory_space=pltpu.VMEM)
    hbm = pl.BlockSpec(memory_space=ANY)
    dma = pltpu.SemaphoreType.DMA
    sds = jax.ShapeDtypeStruct

    def device_step(x_loc, w_router, idx_loc, slot_loc, gelu_loc, lin_loc, out_loc, dy_loc):
        tokens, d_model = x_loc.shape
        exp_local = gelu_loc.shape[0]
        part = gelu_loc.shape[2]
        width = part * n_tp
        experts = exp_local * n_ep
        cap = 4 * tokens // experts
        slots = experts * cap
        s = lax.axis_index("tp")
        idx_t = idx_loc.T
        slot_t = slot_loc.T
        kept = slot_t < cap
        key_t = jnp.where(kept, idx_t * cap + slot_t, -1)
        pos = jnp.where(kept, ((idx_t % n_tp) * n_ep + idx_t // n_tp) * cap + slot_t, slots).reshape(-1)
        wgt = w_router.T
        side = pltpu.CompilerParams(has_side_effects=True, vmem_limit_bytes=VMEM_LIMIT)

        rows, drows, w0, w1, wo, prob, gate, stat, dy_cols, gate_cols = pl.pallas_call(
            functools.partial(dispatch_kernel, n_tp, n_ep, cap),
            name="moe_dispatch",
            out_shape=(sds((n_ep, cap, d_model), BF16), sds((n_ep, cap, d_model), BF16),
                       sds(gelu_loc.shape, BF16), sds(lin_loc.shape, BF16), sds(out_loc.shape, BF16),
                       sds((experts, tokens), F32), sds((8, tokens), F32), sds((n_ep, experts, 128), F32),
                       sds((tokens, 128), BF16), sds((tokens, 8), F32)),
            in_specs=[hbm] * 2 + [vmem] * 3 + [hbm] * 3,
            out_specs=(hbm, hbm, hbm, hbm, hbm, vmem, vmem, vmem, vmem, vmem),
            scratch_shapes=[pltpu.VMEM((tokens, d_model), BF16), pltpu.VMEM((tokens, d_model), BF16),
                            pltpu.VMEM((n_ep, cap, d_model), BF16), pltpu.VMEM((n_ep, cap, d_model), BF16),
                            pltpu.VMEM((experts, 128), F32), pltpu.VMEM((cap, d_model), F32), pltpu.VMEM((cap, d_model), F32),
                            dma((3, n_tp)), dma((3, n_tp)), dma((2, n_ep)), dma((2, n_ep)), dma((n_ep,)), dma((n_ep,)), dma((8,))],
            compiler_params=side,
        )(x_loc, dy_loc, idx_t, key_t, wgt, gelu_loc, lin_loc, out_loc)

        half_shape = lambda ref: sds((n_tp // 2,) + ref.shape[1:], BF16)
        one_shape = lambda ref: sds(ref.shape[1:], BF16)
        table, g0, g1, go, p0, p1, po, n0, n1, no = pl.pallas_call(
            functools.partial(expert_kernel, n_tp, n_ep),
            name="moe_expert",
            out_shape=(sds((n_tp * n_ep, cap, 128), BF16), sds(gelu_loc.shape, BF16), sds(lin_loc.shape, BF16), sds(out_loc.shape, BF16),
                       half_shape(gelu_loc), half_shape(lin_loc), half_shape(out_loc), one_shape(gelu_loc), one_shape(lin_loc), one_shape(out_loc)),
            in_specs=[vmem] * 5,
            out_specs=(hbm, vmem, vmem, vmem) + (hbm,) * 6,
            scratch_shapes=[pltpu.VMEM((d_model, width), BF16), pltpu.VMEM((d_model, width), BF16),
                            pltpu.VMEM((cap // 2, width), BF16), pltpu.VMEM((cap // 2, width), BF16), pltpu.VMEM((cap // 2, width), BF16),
                            pltpu.VMEM((d_model, width), F32), pltpu.VMEM((d_model, width), F32), pltpu.VMEM((width, d_model), F32),
                            pltpu.VMEM((n_tp, n_ep, cap, 128), BF16),
                            dma((2, n_tp, n_ep)), dma((2, n_tp, n_ep)), dma((2,)), dma((3, n_tp // 2)), dma((3, n_tp // 2)), dma((3,)), dma((3,))],
            compiler_params=side,
        )(rows, drows, w0, w1, wo.reshape(width, d_model))

        gy, gx, grad_gelu, grad_lin, grad_out, dwg_t, aux = pl.pallas_call(
            functools.partial(return_kernel, n_tp, n_ep),
            name="moe_return",
            out_shape=(sds((n_tp, tokens // 2, 128), BF16), sds((n_tp, tokens // 2, 128), BF16),
                       sds(gelu_loc.shape, BF16), sds(lin_loc.shape, BF16), sds(out_loc.shape, BF16),
                       sds((experts, d_model), F32), sds((1, 1), F32)),
            in_specs=[pl.BlockSpec(memory_space=pltpu.SMEM)] + [vmem] * 7 + [hbm] * 11,
            out_specs=(hbm, hbm, hbm, hbm, hbm, vmem, pl.BlockSpec(memory_space=pltpu.SMEM)),
            scratch_shapes=[pltpu.VMEM((n_tp * n_ep, cap, 128), BF16), pltpu.VMEM((slots + 8, 128), F32),
                            pltpu.VMEM((tokens, 128), F32), pltpu.VMEM((tokens, 128), F32),
                            pltpu.VMEM((tokens // 2, 128), BF16), pltpu.VMEM((tokens // 2, 128), F32), pltpu.VMEM((8, tokens // 4), F32),
                            pltpu.VMEM((tokens, d_model), BF16), dma((8,)),
                            pltpu.VMEM((n_tp, 8, tokens // 4), F32), pltpu.VMEM((tokens // 2, 128), BF16),
                            pltpu.VMEM((3 * experts, tokens), BF16), pltpu.VMEM((experts, d_model), F32), pltpu.VMEM((n_ep, experts, d_model), F32),
                            pltpu.VMEM((2, 3, d_model, part), BF16), pltpu.VMEM((3, part, d_model), BF16),
                            dma((3, 2, n_tp // 2)), dma((3, 2, n_tp // 2)), dma((3, 6)), dma((n_tp,)), dma((n_tp,)),
                            dma((4, n_tp, 3)), dma((4, n_tp)), dma((4,)), dma((n_ep,)), dma((n_ep,)), dma((8,))],
            compiler_params=side,
        )(pos, gate_cols, dy_cols, prob, gate, idx_t, stat, wgt, table, x_loc, g0, g1, go, p0, p1, po, n0, n1, no)

        pair = pl.BlockSpec((2, tokens // 2, 128), lambda j: (j, 0, 0))
        cols = pl.BlockSpec((tokens, 128), lambda j: (0, j))
        block = lambda ref: pl.BlockSpec((2,) + ref.shape[1:], lambda j: (j, 0, 0))
        y_loc, dx_loc, grad_gelu, grad_lin, grad_out = pl.pallas_call(
            interleave_kernel,
            name="moe_interleave",
            grid=(n_tp // 2,),
            out_shape=(sds((tokens, d_model), BF16), sds((tokens, d_model), BF16), sds(gelu_loc.shape, BF16), sds(lin_loc.shape, BF16), sds(out_loc.shape, BF16)),
            in_specs=[pair, pair, block(gelu_loc), block(lin_loc), block(out_loc)],
            out_specs=(cols, cols, block(gelu_loc), block(lin_loc), block(out_loc)),
            compiler_params=pltpu.CompilerParams(dimension_semantics=("arbitrary",), vmem_limit_bytes=VMEM_LIMIT),
        )(gy, gx, grad_gelu, grad_lin, grad_out)
        return y_loc, dx_loc, grad_gelu, grad_lin, grad_out, dwg_t.T, aux.reshape(())

    rows_spec = P("ep", None)
    weight_in = P("ep", None, "tp")
    weight_out = P("ep", "tp", None)
    return jax.shard_map(
        device_step,
        mesh=mesh,
        in_specs=(rows_spec, P(None, None), rows_spec, rows_spec, weight_in, weight_in, weight_out, rows_spec),
        out_specs=(rows_spec, rows_spec, weight_in, weight_in, weight_out, P(None, None), P()),
        check_vma=False,
    )
```
